32 devices in a mesh: group: 8 (over z, x), tensor: 4 (over y, core).
Axes of the slice: x: 2, y: 2, z: 4, core: 2. Of those that a mesh axis runs over, the one named last changes fastest.
Arguments:
- queries: bfloat16 [1024, 4096], P('group', 'tensor'), may hold values from -120 to 120
- keys: bfloat16 [1024, 512], P('group', 'tensor'), may hold values from -6 to 6
- values: bfloat16 [1024, 512], P('group', 'tensor'), may hold values from -6 to 6
- document_index: int32 [8, 128], P('group'), may hold values from 0 to 7, never falling along the last dimension, each value on 1 to 64 neighbouring positions
- out_proj: bfloat16 [4096, 4096], P('tensor', 'group'), may hold values from -0.25 to 0.25
- residual_in: bfloat16 [1024, 4096], P(('group', 'tensor')), may hold values from -60 to 60
- norm_gain: float32 [4096], replicated, may hold values from 0.1 to 1.9
- expert_ids: int32 [1024, 8], P(('group', 'tensor')), may hold values from 0 to 31, all different within a row; in each aligned block of 32 rows (0 to 31, 32 to 63, ...) at most 16 rows name the same one
- gate_weights: float32 [1024, 8], P(('group', 'tensor')), may hold values from 0.05 to 0.45
- w_gate_up: bfloat16 [32, 4096, 1536], P(('group', 'tensor')), may hold values from -0.09375 to 0.09375
- w_down: bfloat16 [32, 768, 4096], P(('group', 'tensor')), may hold values from -0.21875 to 0.21875
Outputs:
- layer_out: bfloat16 [1024, 4096], P(('group', 'tensor'))
The draws below stay inside these ranges and needn't reach their ends.
Inputs may be any that keep to these rules, and one draw needn't show every extreme that they name: `document_index`: ids never fall along a group's tokens; equal ids mark one document. `expert_ids`: a token names 8 different experts; among the 32 tokens of one device (aligned blocks of rows) no expert is named more than 16 times, a bound that some block reaches.
All inputs are finite; a program needn't handle non-finite values.
Results may differ from the reference program's by a relative error of at most 0.0045.
Values may be sent and summed in bfloat16 or wider, within the bound.
A program may use at most 128 MiB of HBM per device.

```python
import math
import jax
import jax.numpy as jnp
import numpy as np
from jax import lax

D = 4096
QUERY_HEADS = 32
KEY_VALUE_HEADS = 4
HEAD_SIZE = 128
FF = 768
TOPK = 8
TOK_DEV = 32
GROUP_TOKENS = 128
TOTAL_TOKENS = 1024
EXPERTS = 32
CAP = 16
DOCS = 8
N_GROUP = 8


def draw_queries(key, part):
    final_output = jnp.clip(jax.random.normal(jax.random.fold_in(key, 1), (TOTAL_TOKENS, QUERY_HEADS * HEAD_SIZE), jnp.float32), -6.0, 6.0)
    return final_output.astype(jnp.bfloat16)


def draw_keys(key, part):
    final_output = jnp.clip(jax.random.normal(jax.random.fold_in(key, 2), (TOTAL_TOKENS, KEY_VALUE_HEADS * HEAD_SIZE), jnp.float32), -6.0, 6.0)
    return final_output.astype(jnp.bfloat16)


def draw_residual_in(key, part):
    row_scale = jnp.exp(jax.random.uniform(jax.random.fold_in(key, 11), (TOTAL_TOKENS, 1), jnp.float32, jnp.log(0.3), jnp.log(3.0)))
    column_scale = jnp.exp(jax.random.uniform(jax.random.fold_in(key, 12), (1, D), jnp.float32, jnp.log(0.3), jnp.log(3.0)))
    drawn_result = jnp.clip(jax.random.normal(jax.random.fold_in(key, 13), (TOTAL_TOKENS, D), jnp.float32), -6.0, 6.0)
    final_output = drawn_result * row_scale * column_scale
    return final_output.astype(jnp.bfloat16)


def block_scale(own_key, extent, split, low, largest):
    loudness = 1.0
    for dim, parts in split:
        draws = jax.random.uniform(jax.random.fold_in(jax.random.fold_in(own_key, 6), dim), (parts,), jnp.float32, low / len(split), largest / len(split))
        loudness = loudness * jnp.repeat(jnp.exp(draws), extent[dim] // parts).reshape((-1,) + (1,) * (len(extent) - 1 - dim))
    return loudness


def length_profile(number_of, total, limit, skew):
    portions = [(1 << 20) // math.isqrt(grade ** skew) + 1 for grade in range(2, number_of + 1)]
    surplus, given = total - limit - (number_of - 1), [1] * (number_of - 1)
    while surplus > 0:
        movable = [i for i in range(number_of - 1) if given[i] < limit]
        mass, remaining = sum([portions[i] for i in movable]), surplus
        for i in movable:
            more = min(limit - given[i], max(1, remaining * portions[i] // mass), surplus)
            given[i] = given[i] + more
            surplus = surplus - more
    return np.array([limit] + given)


def ragged_sizes(rng, number_of, total, bound, lean):
    if number_of == 2:
        one = jax.random.randint(rng, (), max(1, total - bound), min(bound, total - 1) + 1)
        return jnp.stack([one, total - one])
    sizes = jnp.asarray(length_profile(number_of, total, bound, lean), jnp.int32)
    couples = (number_of - 1) // 2
    donor, receiver = sizes[1:1 + 2 * couples:2], sizes[2:2 + 2 * couples:2]
    slack = jnp.minimum(donor - 1, bound - receiver)
    passed = jax.random.randint(jax.random.fold_in(rng, 1), (couples,), 0, 1 << 20) % (slack + 1)
    sizes = sizes.at[1:1 + 2 * couples:2].set(donor - passed).at[2:2 + 2 * couples:2].set(receiver + passed)
    return sizes[jax.random.permutation(jax.random.fold_in(rng, 2), number_of)]


def shared_out(own_key, own, number, rows, number_of, top, limit, slope):
    sequence = jax.random.permutation(own_key, number_of)
    packed, usual = shares(number_of, rows * top, limit, slope, True), shares(number_of, rows * top, limit, slope, False)
    places = jnp.arange(number_of)

    def named(tallies, offset_by):
        used = int((tallies > 0).sum())
        fixed = max(1, used // 4)
        passed = fixed + (places - fixed + offset_by * (used - fixed)) % max(1, number_of - fixed)
        return jnp.zeros((number_of,), jnp.int32).at[sequence[jnp.where(places < fixed, places, passed)]].set(jnp.asarray(tallies, jnp.int32))

    tallies = jnp.where(number % 4 == 0, named(packed, number // 4), named(usual, number - number // 4 - 1))
    mixed = jax.random.permutation(jax.random.fold_in(own, 3), number_of)
    donor, receiver = mixed[0:number_of // 2 * 2:2], mixed[1:number_of // 2 * 2:2]
    room = jnp.minimum(tallies[donor] - 1, limit - tallies[receiver]) // 2
    room = jnp.where((donor == sequence[0]) | (receiver == sequence[0]) | (tallies[receiver] == 0), 0, jnp.maximum(room, 0))
    passed = jax.random.randint(jax.random.fold_in(own, 4), (number_of // 2,), 0, 1 << 20) % (room + 1)
    tallies = tallies.at[donor].add(-passed).at[receiver].add(passed)
    items = jnp.searchsorted(jnp.cumsum(tallies), jnp.arange(rows * top), side="right").astype(jnp.int32)
    table = items.reshape(top, rows).T
    table = table[jax.random.permutation(jax.random.fold_in(own, 1), rows)]
    offset_by = jax.random.randint(jax.random.fold_in(own, 2), (rows, 1), 0, top)
    return jnp.take_along_axis(table, (jnp.arange(top)[None, :] + offset_by) % top, axis=1)


def shares(amount, total, limit, lean, full):
    portions = [(1 << 20) // math.isqrt(grade ** lean) + 1 for grade in range(1, amount + 1)]
    largest = limit if full else min(limit, max(-(-total // amount), total * portions[0] // sum(portions)))
    least = 1 if total - largest >= amount - 1 else 0
    counts, rest = [largest] + [least] * (amount - 1), total - largest - least * (amount - 1)
    while rest > 0:
        candidates = [i for i in range(1, amount) if counts[i] < largest] or [i for i in range(1, amount) if counts[i] < limit]
        whole, budget = sum([portions[i] for i in candidates]), rest
        for i in candidates:
            extra = min(limit - counts[i], max(1, budget * portions[i] // whole), rest)
            counts[i] = counts[i] + extra
            rest = rest - extra
    return np.array(counts)


def scatter_about(rng, shape, width, reach, shards=(), kind=jnp.bfloat16):
    entries = width * jax.random.normal(rng, shape, jnp.float32)
    if shards:
        entries = entries * block_scale(rng, shape, shards, -0.22, 0.18)
    return jnp.clip(entries, -reach, reach).astype(kind)


def setup_inputs(seed: int = 0) -> dict:
    streams_of = jax.random.split(jax.random.key(seed), 12)
    queries = draw_queries(jax.random.fold_in(streams_of[11], 71), 0)
    keys = draw_keys(jax.random.fold_in(streams_of[11], 71), 0)
    values = scatter_about(streams_of[2], (TOTAL_TOKENS, KEY_VALUE_HEADS * HEAD_SIZE), 1.0, 6.0, ((0, 8), (1, 4)))
    document_index = jax.vmap(lambda own: jnp.searchsorted(jnp.cumsum(ragged_sizes(own, DOCS, GROUP_TOKENS, GROUP_TOKENS // 2, 2)), jnp.arange(GROUP_TOKENS), side="right"))(jax.random.split(streams_of[3], N_GROUP)).reshape((N_GROUP, GROUP_TOKENS)).astype(jnp.int32)
    out_proj = scatter_about(streams_of[4], (QUERY_HEADS * HEAD_SIZE, D), (QUERY_HEADS * HEAD_SIZE // 8) ** -0.5, 0.25, ((0, 4), (1, 8)))
    residual_in = draw_residual_in(jax.random.fold_in(streams_of[11], 71), 0)
    norm_gain = jnp.clip(1.0 + 0.18 * jax.random.normal(streams_of[6], (D,), jnp.float32), 0.1, 1.9)
    expert_ids_keys = jax.random.split(jax.random.fold_in(streams_of[7], 1), TOTAL_TOKENS // TOK_DEV)
    expert_ids_turns = jax.random.permutation(jax.random.fold_in(streams_of[7], 3), TOTAL_TOKENS // TOK_DEV)
    expert_ids = jax.vmap(lambda own, number: shared_out(jax.random.fold_in(streams_of[7], 2), own, number, TOK_DEV, EXPERTS, TOPK, CAP, 2))(expert_ids_keys, expert_ids_turns).reshape((TOTAL_TOKENS, TOPK))
    gate_weights = jnp.clip(0.05 + 0.39999999 * jax.random.uniform(streams_of[8], (TOTAL_TOKENS, TOPK), jnp.float32) ** block_scale(streams_of[8], (TOTAL_TOKENS, TOPK), ((0, 32),), -0.2, 0.2), 0.05, 0.45)
    w_gate_up = scatter_about(streams_of[9], (EXPERTS, D, 2 * FF), D ** -0.5, 0.09375, ((0, 32),))
    w_down = scatter_about(streams_of[10], (EXPERTS, FF, D), FF ** -0.5, 0.21875, ((0, 32),))
    return dict(queries=queries, keys=keys, values=values, document_index=document_index, out_proj=out_proj, residual_in=residual_in, norm_gain=norm_gain, expert_ids=expert_ids, gate_weights=gate_weights, w_gate_up=w_gate_up, w_down=w_down)


def attend(query_matrix, key_matrix, value_matrix, doc_row):
    token_group = query_matrix.shape[0]
    query_head_split = query_matrix.reshape(token_group, KEY_VALUE_HEADS, QUERY_HEADS // KEY_VALUE_HEADS, HEAD_SIZE).astype(jnp.float32)
    key_head_split = key_matrix.reshape(token_group, KEY_VALUE_HEADS, HEAD_SIZE).astype(jnp.float32)
    value_head_split = value_matrix.reshape(token_group, KEY_VALUE_HEADS, HEAD_SIZE).astype(jnp.float32)
    scores = jnp.einsum('qgrd,kgd->grqk', query_head_split, key_head_split) * (1.0 / HEAD_SIZE ** 0.5)
    positions = jnp.arange(token_group, dtype=jnp.int32)
    visible = (positions[:, None] >= positions[None, :]) & (doc_row[:, None] == doc_row[None, :])
    scores = jnp.where(visible, scores, -jnp.inf)
    row_max = lax.optimization_barrier(jnp.max(scores, axis=-1, keepdims=True))
    exponent = jnp.where(visible, jnp.exp(scores - row_max), 0.0)
    weights = (exponent / lax.optimization_barrier(jnp.sum(exponent, axis=-1, keepdims=True))).astype(jnp.bfloat16)
    head_out = jnp.einsum('grqk,kgd->qgrd', weights.astype(jnp.float32), value_head_split)
    return head_out.astype(jnp.bfloat16).reshape(token_group, QUERY_HEADS * HEAD_SIZE)

def reference(queries, keys, values, document_index, out_proj, residual_in, norm_gain, expert_ids, gate_weights, w_gate_up, w_down):
    head_grouped = (queries.reshape(N_GROUP, GROUP_TOKENS, QUERY_HEADS * HEAD_SIZE), keys.reshape(N_GROUP, GROUP_TOKENS, KEY_VALUE_HEADS * HEAD_SIZE), values.reshape(N_GROUP, GROUP_TOKENS, KEY_VALUE_HEADS * HEAD_SIZE), document_index)

    def per_group(inputs):
        return attend(inputs[0], inputs[1], inputs[2], inputs[3])
    head_out = lax.map(per_group, head_grouped).reshape(TOTAL_TOKENS, QUERY_HEADS * HEAD_SIZE)
    hidden = residual_in.astype(jnp.float32) + jnp.dot(head_out, out_proj, preferred_element_type=jnp.float32)
    mean_square = lax.optimization_barrier(jnp.mean(hidden * hidden, axis=-1, keepdims=True))
    normed = (hidden * lax.rsqrt(mean_square + 1e-06) * norm_gain.astype(jnp.float32)).astype(jnp.bfloat16)
    flat_ids = expert_ids.reshape(-1).astype(jnp.int32)
    flat_gate = gate_weights.reshape(-1).astype(jnp.float32)
    token_index = (jnp.arange(TOTAL_TOKENS * TOPK, dtype=jnp.int32) // TOPK).astype(jnp.int32)
    slot_rows = EXPERTS * CAP

    def per_expert(moe_total, inputs):
        expert, gate_up, down_rows = inputs
        chosen = flat_ids == expert
        position = jnp.cumsum(chosen.astype(jnp.int32)) - 1
        position = jnp.where(chosen, position, slot_rows).astype(jnp.int32)
        sources = jnp.zeros((slot_rows,), jnp.int32).at[position].set(token_index, mode='drop')
        weight = jnp.zeros((slot_rows,), jnp.float32).at[position].set(flat_gate, mode='drop')
        gathered_rows = normed[sources]
        projected = jnp.dot(gathered_rows, gate_up, preferred_element_type=jnp.float32)
        activated = (jax.nn.silu(projected[:, :FF]) * projected[:, FF:]).astype(jnp.bfloat16)
        expert_out = jnp.dot(activated, down_rows, preferred_element_type=jnp.float32).astype(jnp.bfloat16)
        moe_total = moe_total.at[sources].add(expert_out.astype(jnp.float32) * weight[:, None])
        return (moe_total, None)
    moe_total, _ = lax.scan(per_expert, jnp.zeros((TOTAL_TOKENS, D), jnp.float32), (jnp.arange(EXPERTS, dtype=jnp.int32), w_gate_up, w_down))
    return (hidden + moe_total).astype(jnp.bfloat16)
```

```python
import functools

import jax
import jax.numpy as jnp
from jax import lax
from jax.experimental import pallas as pl
from jax.experimental.pallas import tpu as pltpu
from jax.sharding import PartitionSpec as P

HEAD_SIZE = 128
LANES = 128
MESH = pl.DeviceIdType.MESH
VMEM_LIMIT = 62 * 1024 * 1024
F32 = jnp.float32
BF16 = jnp.bfloat16


def attention(queries, keys, values, document_index):
    token_group = queries.shape[0]
    kv_dev = keys.shape[1] // HEAD_SIZE
    query_dev = queries.shape[1] // HEAD_SIZE
    group_ratio = query_dev // kv_dev
    query_head_split = queries.reshape(token_group, kv_dev, group_ratio, HEAD_SIZE)
    key_head_split = keys.reshape(token_group, kv_dev, HEAD_SIZE)
    value_head_split = values.reshape(token_group, kv_dev, HEAD_SIZE)
    scores = jnp.einsum(
        "qgrd,kgd->grqk", query_head_split, key_head_split, preferred_element_type=F32
    ) * (1.0 / HEAD_SIZE**0.5)
    doc_row = document_index[0]
    positions = jnp.arange(token_group, dtype=jnp.int32)
    visible = (positions[:, None] >= positions[None, :]) & (doc_row[:, None] == doc_row[None, :])
    scores = jnp.where(visible, scores, -jnp.inf)
    row_max = jnp.max(scores, axis=-1, keepdims=True)
    exponent = jnp.where(visible, jnp.exp(scores - row_max), 0.0)
    weights = (exponent / jnp.sum(exponent, axis=-1, keepdims=True)).astype(BF16)
    head_out = jnp.einsum("grqk,kgd->qgrd", weights, value_head_split, preferred_element_type=F32)
    return head_out.astype(BF16).reshape(token_group, query_dev * HEAD_SIZE)


def device(z, x, y, c):
    return (z * 2 + x, y * 2 + c)


def layer_kernel(
    slabs,
    copies_max,
    head_ref,
    proj_ref,
    res_ref,
    gain_ref,
    gate_ref,
    gate_up_hbm,
    down_hbm,
    out_ref,
    proj_x,
    heads,
    res_in,
    part,
    got_half,
    sum_half,
    got_y,
    gates,
    rows,
    scaled,
    squares,
    acc,
    act,
    gate_up,
    down,
    hidden,
    got_core,
    got_a,
    got_b,
    last_a,
    last_b,
    landed,
    load_sem,
    send_sems,
    recv_sems,
):
    g, t = lax.axis_index("group"), lax.axis_index("tensor")
    z, x, y, c = g // 2, g % 2, t // 2, t % 2
    tok, model = res_ref.shape
    plane = model // slabs
    width = plane // 2
    ff2 = gate_up.shape[2]
    ff = ff2 // 2
    experts = slabs * 8
    block = slabs * tok
    after = [lax.rem(z + j, slabs) for j in range(slabs)]
    before = [lax.rem(z + slabs - j, slabs) for j in range(slabs)]
    core, over_y, over_x = device(z, x, y, 1 - c), device(z, x, 1 - y, c), device(z, 1 - x, y, c)
    up = [device(before[j], x, y, c) for j in range(slabs)]
    own_cols = pl.ds(pl.multiple_of(x * width, width), width)
    other_cols = pl.ds(pl.multiple_of((1 - x) * width, width), width)

    loads = [
        pltpu.make_async_copy(
            gate_up_hbm.at[pl.ds(pl.multiple_of(after[j] * plane, plane), plane)],
            gate_up.at[j],
            load_sem.at[j],
        )
        for j in range(slabs)
    ]
    loads.append(pltpu.make_async_copy(down_hbm, down, load_sem.at[slabs]))
    for load in loads:
        load.start()

    barrier = pltpu.get_barrier_semaphore()
    partners = [core, over_y, over_x] + up[1:]
    for partner in partners:
        pl.semaphore_signal(barrier, inc=1, device_id=partner, device_id_type=MESH)
    pl.semaphore_wait(barrier, len(partners))

    count = [0]
    pending = []

    def send(src, dst, target):
        k = count[0]
        count[0] = k + 1
        copy = pltpu.make_async_remote_copy(
            src_ref=src,
            dst_ref=dst,
            send_sem=send_sems.at[k],
            recv_sem=recv_sems.at[k],
            device_id=target,
            device_id_type=MESH,
        )
        copy.start()
        pending.append(copy)
        return copy

    proj_copy = send(proj_ref, proj_x, over_x)
    head_copy = [None] + [send(head_ref, heads.at[j - 1], up[j]) for j in range(1, slabs)]
    res_copy = [None] + [
        send(
            res_ref.at[:, pl.ds(pl.multiple_of(before[j] * plane, plane), plane)],
            res_in.at[j - 1],
            up[j],
        )
        for j in range(1, slabs)
    ]
    gate_copy = [send(gate_ref, gates.at[z, x, y, c], up[j]) for j in range(1, slabs)]
    gates[z, x, y, c] = gate_ref[...]
    squares[...] = jnp.zeros_like(squares)

    def project(j, weights, columns):
        source = head_ref if j == 0 else heads.at[j - 1]
        got = jnp.dot(source[...], weights[...], preferred_element_type=F32)
        for yy in range(2):
            for cc in range(2):
                start = (yy * 2 + cc) * tok
                part[j, cc, yy, :, columns] = got[start : start + tok]

    half_copy, y_copy = {}, {}

    def over_cores(j):
        half_copy[j].wait_recv()
        total = part[j, c, 1 - y] + got_half[j, 1 - y]
        sum_half[j] = total.astype(BF16)
        y_copy[j] = send(sum_half.at[j], got_y.at[j], over_y)
        part[j, c, y] = part[j, c, y] + got_half[j, y]

    def finish(j):
        y_copy[j].wait_recv()
        if j:
            res_copy[j].wait_recv()
            residual = res_in[j - 1]
        else:
            residual = res_ref[:, pl.ds(pl.multiple_of(z * plane, plane), plane)]
        total = residual.astype(F32) + (part[j, c, y] + got_y[j].astype(F32))
        spot = pl.ds(pl.multiple_of(after[j] * tok, tok), tok)
        rows[z, x, y, c, spot, :] = total.astype(BF16)

    for j in range(slabs):
        if j:
            head_copy[j].wait_recv()
        project(j, proj_ref, own_cols)
    for copy in gate_copy:
        copy.wait_recv()
    gate_x = send(gates.at[:, x, y, c], gates.at[:, x, y, c], over_x)
    proj_copy.wait_recv()
    for j in range(slabs):
        project(j, proj_x, other_cols)
        half_copy[j] = send(part.at[j, 1 - c], got_half.at[j], core)
        if j >= 1:
            over_cores(j - 1)
    over_cores(slabs - 1)
    for j in range(slabs):
        finish(j)

    low, high = pl.ds(0, width), pl.ds(width, width)
    g_copy = {}
    g_start = len(pending)

    def pass_on(kind, j, spot, target):
        g_copy[kind, j] = send(spot, spot, target)

    for j in range(1, slabs):
        pass_on(0, j, rows.at[z, x, y, c], up[j])

    def first(j):
        if j:
            g_copy[0, j].wait_recv()
        pass_on(1, j, rows.at[after[j], x, y, c, :, low], over_x)
        pass_on(2, j, rows.at[after[j], x, y, c, :, high], over_y)
        pass_on(3, j, rows.at[after[j], x, y, c], core)

    def second(j):
        g_copy[1, j].wait_recv()
        pass_on(4, j, rows.at[after[j], :, y, c, :, low], over_y)
        pass_on(5, j, rows.at[after[j], 1 - x, y, c, :, low], core)
        g_copy[2, j].wait_recv()
        pass_on(6, j, rows.at[after[j], x, :, c, :, high], over_x)
        pass_on(7, j, rows.at[after[j], x, 1 - y, c, :, high], core)

    def third(j):
        g_copy[4, j].wait_recv()
        pass_on(8, j, rows.at[after[j], :, 1 - y, c, :, low], core)
        g_copy[6, j].wait_recv()
        pass_on(9, j, rows.at[after[j], 1 - x, :, c, :, high], core)

    def up_project(j):
        for kind in (3, 5, 7, 8, 9):
            g_copy[kind, j].wait_recv()
        p = after[j]
        gain_cols = pl.ds(pl.multiple_of(p * plane, plane), plane)

        @pl.loop(0, 8)
        def _(b):
            @pl.loop(0, slabs)
            def _(s):
                spot = pl.ds(pl.multiple_of(s * tok, tok), tok)
                value = rows[p, b // 4, (b // 2) % 2, b % 2, spot, :].astype(F32)
                place = pl.ds(pl.multiple_of(b * block + s * tok, tok), tok)
                square = squares[place, :]
                for lane in range(plane // LANES):
                    piece = value[:, lane * LANES : (lane + 1) * LANES]
                    square = square + piece * piece
                squares[place, :] = square
                scaled[place, :] = (value * gain_ref[:, gain_cols]).astype(BF16)

        loads[j].wait()
        step = 512

        @pl.loop(0, ff2 // step)
        def _(n):
            columns = pl.ds(pl.multiple_of(n * step, step), step)
            got = jnp.dot(
                scaled[...], gate_up[j, :, columns], preferred_element_type=F32
            )
            if j:
                acc[:, columns] = acc[:, columns] + got
            else:
                acc[:, columns] = got

    first(0)
    gate_x.wait_recv()
    gate_y = send(gates.at[:, :, y, c], gates.at[:, :, y, c], over_y)
    second(0)
    if slabs > 1:
        first(1)
    third(0)
    gate_y.wait_recv()
    gate_c = send(gates.at[:, :, :, c], gates.at[:, :, :, c], core)
    for j in range(slabs):
        if j + 1 < slabs:
            second(j + 1)
        if j + 2 < slabs:
            first(j + 2)
        up_project(j)
        if j + 1 < slabs:
            third(j + 1)
    gate_c.wait_recv()
    own = pl.ds(pl.multiple_of(z * tok, tok), tok)
    for q in range(slabs):
        hidden[q] = rows[q, x, y, c, own, :]
    for copy in pending[g_start:]:
        copy.wait_send()
    g_end = len(pending)
    loads[slabs].wait()

    me = g * 4 + t
    lane = lax.broadcasted_iota(jnp.int32, (tok, LANES), 1)
    picked = (lane == me) | (lane == me + experts)
    halves = slabs // 2
    quarters = [pl.ds(0, halves), pl.ds(halves, slabs - halves)]

    def spots(j):
        return pl.ds(j * tok, tok)

    c_copy, a_copy, b_copy, la_copy, lb_copy, z_copy = {}, {}, {}, {}, {}, {}

    def down_project(j):
        p = after[j]
        for cc in range(2):
            for xx in range(2):
                for yy in range(2):
                    source = c if cc == 0 else 1 - c
                    b = xx * 4 + yy * 2 + source
                    place = pl.ds(pl.multiple_of(b * block + p * tok, tok), tok)
                    mean = jnp.sum(squares[place, :], axis=-1, keepdims=True) * (1.0 / model)
                    scale = lax.rsqrt(mean + 1e-06)
                    gate = jnp.sum(
                        jnp.where(picked, gates[p, xx, yy, source].astype(F32), 0.0),
                        axis=-1,
                        keepdims=True,
                    )
                    left = acc[place, :ff] * scale
                    right = acc[place, ff:] * (scale * gate)
                    value = left / (1.0 + jnp.exp(-left)) * right
                    spot = ((cc * 2 + xx) * 2 + yy) * tok
                    act[spot : spot + tok, :] = value.astype(BF16)
        step = plane // 2

        @pl.loop(0, model // step)
        def _(n):
            got = jnp.dot(
                act[...],
                down[:, pl.ds(pl.multiple_of(n * step, step), step)],
                preferred_element_type=F32,
            ).astype(BF16)
            columns = pl.ds(pl.multiple_of((n % 2) * step, step), step)
            for cc in range(2):
                for xx in range(2):
                    for yy in range(2):
                        spot = ((cc * 2 + xx) * 2 + yy) * tok
                        rows[n // 2, xx, yy, 1 - cc, spots(j), columns] = got[spot : spot + tok]

        c_copy[j] = [
            send(rows.at[q, :, :, 0, spots(j)], got_core.at[j, q], core) for q in quarters
        ]

    def add_cores(j):
        for h in range(2):
            c_copy[j][h].wait_recv()

            @pl.loop(quarters[h].start, quarters[h].start + quarters[h].size)
            def _(q):
                for xx in range(2):
                    for yy in range(2):
                        total = rows[q, xx, yy, 1, spots(j), :].astype(F32) + got_core[
                            j, q, xx, yy
                        ].astype(F32)
                        rows[q, xx, yy, 1, spots(j), :] = total.astype(BF16)

            if h == 0:
                a_copy[j] = send(
                    rows.at[quarters[0], 1 - x, :, 1, spots(j)], got_a.at[j], over_x
                )
            else:
                b_copy[j] = send(
                    rows.at[quarters[1], :, 1 - y, 1, spots(j)], got_b.at[j], over_y
                )

    def add_second(j):
        a_copy[j].wait_recv()
        for q in range(halves):
            for yy in range(2):
                total = rows[q, x, yy, 1, spots(j), :].astype(F32) + got_a[j, q, yy].astype(F32)
                rows[q, x, yy, 1, spots(j), :] = total.astype(BF16)
        la_copy[j] = send(rows.at[quarters[0], x, 1 - y, 1, spots(j)], last_a.at[j], over_y)
        b_copy[j].wait_recv()
        for q in range(slabs - halves):
            for xx in range(2):
                total = rows[halves + q, xx, y, 1, spots(j), :].astype(F32) + got_b[
                    j, q, xx
                ].astype(F32)
                rows[halves + q, xx, y, 1, spots(j), :] = total.astype(BF16)
        lb_copy[j] = send(rows.at[quarters[1], 1 - x, y, 1, spots(j)], last_b.at[j], over_x)

    def add_third(j):
        la_copy[j].wait_recv()
        lb_copy[j].wait_recv()
        for q in range(slabs):
            last = last_a[j, q] if q < halves else last_b[j, q - halves]
            total = rows[q, x, y, 1, spots(j), :].astype(F32) + last.astype(F32)
            rows[q, x, y, 1, spots(j), :] = total.astype(BF16)
        if j:
            z_copy[j] = send(
                rows.at[:, x, y, 1, spots(j)], landed.at[j - 1], device(after[j], x, y, c)
            )

    order = list(range(1, slabs)) + [0]
    for i, j in enumerate(order):
        down_project(j)
        if i >= 1:
            add_cores(order[i - 1])
        if i >= 2:
            add_second(order[i - 2])
        if i >= 3:
            add_third(order[i - 3])
    add_cores(order[-1])
    for j in order[max(slabs - 2, 0) :]:
        add_second(j)
        if j == order[-1]:
            break
        if slabs >= 3:
            add_third(order[order.index(j) - 1])
    for j in order[max(slabs - 2, 0) :]:
        add_third(j)
    for j in range(1, slabs):
        z_copy[j].wait_recv()
    for q in range(slabs):
        total = hidden[q].astype(F32) + rows[q, x, y, 1, spots(0), :].astype(F32)
        for j in range(1, slabs):
            total = total + landed[j - 1, q].astype(F32)
        out_ref[:, q * plane : (q + 1) * plane] = total.astype(BF16)
    for copy in pending[:g_start] + pending[g_end:]:
        copy.wait_send()
    assert count[0] <= copies_max, count[0]


def layer(head_out, out_proj, residual, gain, gates, gate_up, down, groups):
    slabs = groups // 2
    tok, model = residual.shape
    tokens, depth = head_out.shape
    plane = model // slabs
    ff, ff2 = down.shape[0], gate_up.shape[1]
    total = tok * slabs * 8
    halves = slabs // 2
    copies_max = 128
    dma = pltpu.SemaphoreType.DMA
    vmem = pl.BlockSpec(memory_space=pltpu.VMEM)
    hbm = pl.BlockSpec(memory_space=pl.ANY)
    return pl.pallas_call(
        functools.partial(layer_kernel, slabs, copies_max),
        out_shape=jax.ShapeDtypeStruct((tok, model), BF16),
        in_specs=[vmem] * 5 + [hbm] * 2,
        out_specs=vmem,
        scratch_shapes=[
            pltpu.VMEM(out_proj.shape, BF16),
            pltpu.VMEM((slabs - 1, tokens, depth), BF16),
            pltpu.VMEM((slabs - 1, tok, plane), BF16),
            pltpu.VMEM((slabs, 2, 2, tok, plane), F32),
            pltpu.VMEM((slabs, 2, tok, plane), F32),
            pltpu.VMEM((slabs, tok, plane), BF16),
            pltpu.VMEM((slabs, tok, plane), BF16),
            pltpu.VMEM((slabs, 2, 2, 2, tok, LANES), BF16),
            pltpu.VMEM((slabs, 2, 2, 2, slabs * tok, plane), BF16),
            pltpu.VMEM((total, plane), BF16),
            pltpu.VMEM((total, LANES), F32),
            pltpu.VMEM((total, ff2), F32),
            pltpu.VMEM((8 * tok, ff), BF16),
            pltpu.VMEM((slabs, plane, ff2), BF16),
            pltpu.VMEM((ff, model), BF16),
            pltpu.VMEM((slabs, tok, plane), BF16),
            pltpu.VMEM((slabs, slabs, 2, 2, tok, plane), BF16),
            pltpu.VMEM((slabs, halves, 2, tok, plane), BF16),
            pltpu.VMEM((slabs, slabs - halves, 2, tok, plane), BF16),
            pltpu.VMEM((slabs, halves, tok, plane), BF16),
            pltpu.VMEM((slabs, slabs - halves, tok, plane), BF16),
            pltpu.VMEM((slabs - 1, slabs, tok, plane), BF16),
            dma((slabs + 1,)),
            dma((copies_max,)),
            dma((copies_max,)),
        ],
        compiler_params=pltpu.CompilerParams(
            collective_id=0, has_side_effects=True, vmem_limit_bytes=VMEM_LIMIT
        ),
    )(head_out, out_proj, residual, gain, gates, gate_up, down)


def spread_gates(expert_ids, gate_weights, experts):
    gates = jnp.sum(
        jnp.where(
            expert_ids[:, :, None] == jnp.arange(experts, dtype=jnp.int32)[None, None, :],
            gate_weights[:, :, None],
            0.0,
        ),
        axis=1,
    )
    high = lax.reduce_precision(gates, 8, 7)
    low = gates - high
    pad = -(2 * experts) % LANES
    return jnp.concatenate(
        [high, low, jnp.zeros((gates.shape[0], pad), F32)], axis=1
    ).astype(BF16)


def plain_layer(head_out, out_proj, residual, gain, extra, gate_up, down, groups, tensors):
    experts = groups * tensors
    tok, model = residual.shape
    heads = lax.all_gather(head_out, "group", axis=0, tiled=True)
    part = jnp.dot(heads, out_proj, preferred_element_type=F32)
    part = part.reshape(groups, tensors, tok, part.shape[1])
    part = lax.psum_scatter(part, "tensor", scatter_dimension=1, tiled=False)
    attended = lax.all_to_all(part, "group", split_axis=0, concat_axis=2, tiled=True)
    hidden = residual.astype(F32) + attended.reshape(tok, model)
    mean_square = jnp.mean(hidden * hidden, axis=-1, keepdims=True)
    normed = (hidden * lax.rsqrt(mean_square + 1e-06) * gain).astype(BF16)
    rows = jnp.concatenate([normed, extra], axis=1)
    rows_all = lax.all_gather(rows, ("group", "tensor"), axis=0, tiled=True)
    me = lax.axis_index("group") * tensors + lax.axis_index("tensor")
    lane = jnp.arange(extra.shape[1], dtype=jnp.int32)
    picked = (lane == me) | (lane == me + experts)
    gate_col = jnp.sum(
        jnp.where(picked[None, :], rows_all[:, model:].astype(F32), 0.0), axis=1, keepdims=True
    )
    ff = down.shape[0]
    projected = jnp.dot(rows_all[:, :model], gate_up, preferred_element_type=F32)
    activated = (jax.nn.silu(projected[:, :ff]) * projected[:, ff:]).astype(BF16)
    expert_out = jnp.dot(activated, down, preferred_element_type=F32)
    weighted = (expert_out * gate_col).astype(BF16)
    expert_sum = lax.psum_scatter(weighted, ("group", "tensor"), scatter_dimension=0, tiled=True)
    return (hidden + expert_sum.astype(F32)).astype(BF16)


def on_device(
    queries,
    keys,
    values,
    document_index,
    out_proj,
    residual_in,
    norm_gain,
    expert_ids,
    gate_weights,
    w_gate_up,
    w_down,
):
    groups, tensors = lax.axis_size("group"), lax.axis_size("tensor")
    experts = groups * tensors
    gain = norm_gain[None, :]
    head_out = attention(queries, keys, values, document_index)
    extra = spread_gates(expert_ids, gate_weights, experts)
    if groups == 8 and tensors == 4:
        return layer(
            head_out, out_proj, residual_in, gain, extra, w_gate_up[0], w_down[0], groups
        )
    return plain_layer(
        head_out, out_proj, residual_in, gain, extra, w_gate_up[0], w_down[0], groups, tensors
    )


def solution(mesh):
    in_specs = (
        P("group", "tensor"),
        P("group", "tensor"),
        P("group", "tensor"),
        P("group", None),
        P("tensor", "group"),
        P(("group", "tensor"), None),
        P(),
        P(("group", "tensor"), None),
        P(("group", "tensor"), None),
        P(("group", "tensor"), None, None),
        P(("group", "tensor"), None, None),
    )
    out_specs = P(("group", "tensor"), None)
    return jax.shard_map(
        on_device, mesh=mesh, in_specs=in_specs, out_specs=out_specs, check_vma=False
    )
```

```python
import functools

import jax
import jax.numpy as jnp
from jax import lax
from jax.experimental import pallas as pl
from jax.experimental.pallas import tpu as pltpu
from jax.sharding import PartitionSpec as P

HEAD_SIZE = 128
LANES = 128
MESH = pl.DeviceIdType.MESH
VMEM_LIMIT = 62 * 1024 * 1024
F32 = jnp.float32
BF16 = jnp.bfloat16


def attention(queries, keys, values, document_index):
    token_group = queries.shape[0]
    kv_dev = keys.shape[1] // HEAD_SIZE
    query_dev = queries.shape[1] // HEAD_SIZE
    group_ratio = query_dev // kv_dev
    query_head_split = queries.reshape(token_group, kv_dev, group_ratio, HEAD_SIZE)
    key_head_split = keys.reshape(token_group, kv_dev, HEAD_SIZE)
    value_head_split = values.reshape(token_group, kv_dev, HEAD_SIZE)
    scores = jnp.einsum(
        "qgrd,kgd->grqk", query_head_split, key_head_split, preferred_element_type=F32
    ) * (1.0 / HEAD_SIZE**0.5)
    doc_row = document_index[0]
    positions = jnp.arange(token_group, dtype=jnp.int32)
    visible = (positions[:, None] >= positions[None, :]) & (doc_row[:, None] == doc_row[None, :])
    scores = jnp.where(visible, scores, -jnp.inf)
    row_max = jnp.max(scores, axis=-1, keepdims=True)
    exponent = jnp.where(visible, jnp.exp(scores - row_max), 0.0)
    weights = (exponent / jnp.sum(exponent, axis=-1, keepdims=True)).astype(BF16)
    head_out = jnp.einsum("grqk,kgd->qgrd", weights, value_head_split, preferred_element_type=F32)
    return head_out.astype(BF16).reshape(token_group, query_dev * HEAD_SIZE)


def device(z, x, y, c):
    return (z * 2 + x, y * 2 + c)


def nearest_first(z):
    first = jnp.where(z == 0, 1, jnp.where(z == 1, 2, jnp.where(z == 2, 1, 2)))
    second = jnp.where(z == 0, 2, jnp.where(z == 1, 0, jnp.where(z == 2, 3, 1)))
    third = jnp.where(z <= 1, 3, 0)
    return [first, second, third]


def layer_kernel(
    slabs,
    copies_max,
    query_hbm,
    key_hbm,
    value_hbm,
    doc_ref,
    proj_hbm,
    res_hbm,
    gain_ref,
    ids_ref,
    weight_ref,
    gate_up_hbm,
    down_hbm,
    out_ref,
    query_ref,
    key_ref,
    value_ref,
    proj_ref,
    res_ref,
    head_own,
    proj_x,
    heads,
    res_in,
    part,
    got_half,
    sum_half,
    got_y,
    gates,
    rows,
    scaled,
    squares,
    acc,
    act,
    gate_up,
    down,
    hidden,
    got_core,
    got_x,
    got_y2,
    last_d,
    last_a,
    landed_a,
    landed_d,
    load_sem,
    send_sems,
    recv_sems,
):
    g, t = lax.axis_index("group"), lax.axis_index("tensor")
    z, x, y, c = g // 2, g % 2, t // 2, t % 2
    tok, model = res_ref.shape
    plane = model // slabs
    width = plane // 2
    ff2 = gate_up.shape[2]
    ff = ff2 // 2
    experts = slabs * 8
    block = slabs * tok
    others = nearest_first(z)
    planes = [z] + others
    core, over_y, over_x = device(z, x, y, 1 - c), device(z, x, 1 - y, c), device(z, 1 - x, y, c)

    def plane_cols(p):
        return pl.ds(pl.multiple_of(p * plane, plane), plane)

    small = [
        pltpu.make_async_copy(source, target, load_sem.at[slabs + 1 + i])
        for i, (source, target) in enumerate(
            [
                (key_hbm, key_ref),
                (query_hbm, query_ref),
                (value_hbm, value_ref),
                (proj_hbm, proj_ref),
                (res_hbm, res_ref),
            ]
        )
    ]
    for load in small:
        load.start()
    barrier = pltpu.get_barrier_semaphore()
    partners = [core, over_y, over_x] + [device(p, x, y, c) for p in others]
    for partner in partners:
        pl.semaphore_signal(barrier, inc=1, device_id=partner, device_id_type=MESH)
    loads = [
        pltpu.make_async_copy(
            gate_up_hbm.at[pl.ds(pl.multiple_of(planes[k] * plane, plane), plane)],
            gate_up.at[k],
            load_sem.at[k],
        )
        for k in range(slabs)
    ]
    loads.append(pltpu.make_async_copy(down_hbm, down, load_sem.at[slabs]))

    lane = lax.broadcasted_iota(jnp.int32, (tok, LANES), 1)
    gate = jnp.zeros((tok, LANES), F32)
    for k in range(ids_ref.shape[1]):
        chosen = ids_ref[:, k : k + 1]
        hit = (lane == chosen) | (lane == chosen + experts)
        gate = gate + jnp.where(hit, weight_ref[:, k : k + 1], 0.0)
    gate_high = gate.astype(BF16).astype(F32)
    gates[z, x, y, c] = jnp.where(lane < experts, gate_high, gate - gate_high).astype(BF16)
    squares[...] = jnp.zeros_like(squares)

    for load in small[:3]:
        load.wait()

    def attend():
        tokens = query_ref.shape[0]
        doc = jnp.broadcast_to(doc_ref[...].astype(F32), (tokens, tokens))
        row = lax.broadcasted_iota(jnp.int32, (tokens, tokens), 0)
        column = lax.broadcasted_iota(jnp.int32, (tokens, tokens), 1)
        visible = (row >= column) & (doc == doc.T)
        for h in range(query_ref.shape[1] // HEAD_SIZE):
            span = slice(h * HEAD_SIZE, (h + 1) * HEAD_SIZE)
            scores = lax.dot_general(
                query_ref[:, span],
                key_ref[...],
                (((1,), (1,)), ((), ())),
                preferred_element_type=F32,
            ) * (1.0 / HEAD_SIZE**0.5)
            scores = jnp.where(visible, scores, -jnp.inf)
            exponent = jnp.exp(scores - jnp.max(scores, axis=-1, keepdims=True))
            total = jnp.sum(exponent, axis=-1, keepdims=True)
            probs = (exponent / total).astype(BF16)
            head_own[:, span] = jnp.dot(
                probs, value_ref[...], preferred_element_type=F32
            ).astype(BF16)

    attend()
    for load in small[3:]:
        load.wait()
    pl.semaphore_wait(barrier, len(partners))
    for load in loads:
        load.start()

    count = [0]
    pending = []

    def copy_of(src, dst, send_index, recv_index, target):
        return pltpu.make_async_remote_copy(
            src_ref=src,
            dst_ref=dst,
            send_sem=send_sems.at[send_index],
            recv_sem=recv_sems.at[recv_index],
            device_id=target,
            device_id_type=MESH,
        )

    def take(n):
        k = count[0]
        count[0] = k + n
        return k

    def send(src, dst, target):
        k = take(1)
        copy = copy_of(src, dst, k, k, target)
        copy.start()
        pending.append(copy)
        return copy

    def send_planes(source, target):
        k = take(slabs)
        for i, p in enumerate(others):
            copy = copy_of(source(p), target(z), k + i, k + z, device(p, x, y, c))
            copy.start()
            pending.append(copy)
        return lambda p: copy_of(target(p), target(p), k, k + p, core)

    pieces = 2
    piece = width // pieces
    proj_copy = []
    for i in range(pieces):
        cols = pl.ds(i * piece, piece)
        proj_copy.append(send(proj_ref.at[:, cols], proj_x.at[:, cols], over_x))
    above = device(jnp.minimum(z + 1, slabs - 1), x, y, c)
    below = device(jnp.maximum(z - 1, 0), x, y, c)
    is_low, is_high = z < slabs - 1, z > 0
    chunks = 2
    chunk = head_own.shape[1] // chunks
    chain = [take(slabs + 2) for _ in range(chunks)]
    spans = [pl.ds(i * chunk, chunk) for i in range(chunks)]

    def own_copy(i, rising):
        return copy_of(
            head_own.at[:, spans[i]],
            heads.at[z, :, spans[i]],
            chain[i] + slabs + (0 if rising else 1),
            chain[i] + z,
            above if rising else below,
        )

    def relay_copy(i, p, target):
        spot = heads.at[p, :, spans[i]]
        return copy_of(spot, spot, chain[i] + p, chain[i] + p, target)

    def chain_do(i, p, act_on):
        if p is None:
            rising, falling = is_low, is_high
        else:
            rising, falling = (p < z) & is_low, (p > z) & is_high

        @pl.when(rising)
        def _():
            act_on(own_copy(i, True) if p is None else relay_copy(i, p, above))

        @pl.when(falling)
        def _():
            act_on(own_copy(i, False) if p is None else relay_copy(i, p, below))

    for i in range(chunks):
        chain_do(i, None, lambda copy: copy.start())

    def relay(p):
        for i in range(chunks):
            relay_copy(i, p, above).wait_recv()
            chain_do(i, p, lambda copy: copy.start())

    def project(k, weights, columns):
        source = head_own[...] if k == 0 else heads[planes[k]]
        got = jnp.dot(source, weights, preferred_element_type=F32)
        for yy in range(2):
            for cc in range(2):
                start = (yy * 2 + cc) * tok
                part[k, cc, yy, :, columns] = got[start : start + tok]

    def columns_of(i):
        if i == 0:
            return pl.ds(pl.multiple_of(x * width, width), width)
        return pl.ds(pl.multiple_of((1 - x) * width + (i - 1) * piece, piece), piece)

    half_copy, y_copy = {}, {}

    def to_core(i, ks):
        columns = columns_of(i)
        half_copy[i, ks] = send(
            part.at[pl.ds(ks[0], len(ks)), 1 - c, :, :, columns],
            got_half.at[pl.ds(ks[0], len(ks)), :, :, columns],
            core,
        )

    def over_cores(i, ks):
        columns = columns_of(i)
        half_copy[i, ks].wait_recv()
        for k in ks:
            total = part[k, c, 1 - y, :, columns] + got_half[k, 1 - y, :, columns]
            sum_half[k, :, columns] = total.astype(BF16)
        spot = pl.ds(ks[0], len(ks))
        y_copy[i, ks] = send(
            sum_half.at[spot, :, columns], got_y.at[spot, :, columns], over_y
        )
        for k in ks:
            part[k, c, y, :, columns] = part[k, c, y, :, columns] + got_half[k, y, :, columns]

    half_tok = tok // 2

    def finish(i, ks):
        columns = columns_of(i)
        y_copy[i, ks].wait_recv()
        for k in ks:
            total = part[k, c, y, :, columns] + got_y[k, :, columns].astype(F32)
            total = (total + res_in[planes[k], :, columns].astype(F32)).astype(BF16)
            spot = pl.ds(pl.multiple_of(planes[k] * half_tok, half_tok), half_tok)
            for h in range(2):
                rows[z, x, y, c, h, spot, columns] = total[h * half_tok : (h + 1) * half_tok]

    every = tuple(range(slabs))
    project(0, proj_ref[...], columns_of(0))
    to_core(0, (0,))
    for k in range(1, slabs):
        relay(planes[k])
        project(k, proj_ref[...], columns_of(0))
        to_core(0, (k,))
    res_wait = send_planes(lambda p: res_ref.at[:, plane_cols(p)], lambda p: res_in.at[p])
    gate_wait = send_planes(lambda p: gates.at[z, x, y, c], lambda p: gates.at[p, x, y, c])
    for k in range(slabs):
        over_cores(0, (k,))
    for i in range(pieces):
        proj_copy[i].wait_recv()
        for k in range(slabs):
            project(k, proj_x[:, i * piece : (i + 1) * piece], columns_of(1 + i))
        to_core(1 + i, every)
        if i == 0:
            res_in[z] = res_ref[:, plane_cols(z)]
        over_cores(1 + i, every)
    for p in others:
        res_wait(p).wait_recv()
    for k in range(slabs):
        finish(0, (k,))
    for i in range(pieces):
        finish(1 + i, every)

    low, high = pl.ds(0, width), pl.ds(width, width)
    g_copy = {}
    g_start = len(pending)
    g_marks = {}

    def pass_on(kind, unit, spot, target):
        g_copy[kind, unit] = send(spot, spot, target)

    z_wait = [
        send_planes(
            lambda p, h=h: rows.at[z, x, y, c, h], lambda p, h=h: rows.at[p, x, y, c, h]
        )
        for h in range(2)
    ]
    for p in others:
        gate_wait(p).wait_recv()
    gate_x = send(gates.at[:, x, y, c], gates.at[:, x, y, c], over_x)

    def first(h, k):
        p = planes[k]
        if k:
            z_wait[h](p).wait_recv()
        pass_on("x", (h, k), rows.at[p, x, y, c, h, :, low], over_x)
        pass_on("y", (h, k), rows.at[p, x, y, c, h, :, high], over_y)
        pass_on("c", (h, k), rows.at[p, x, y, c, h], core)

    def second(h, k):
        p = planes[k]
        g_copy["x", (h, k)].wait_recv()
        pass_on("xy", (h, k), rows.at[p, :, y, c, h, :, low], over_y)
        pass_on("xc", (h, k), rows.at[p, 1 - x, y, c, h, :, low], core)
        g_copy["y", (h, k)].wait_recv()
        pass_on("yx", (h, k), rows.at[p, x, :, c, h, :, high], over_x)
        pass_on("yc", (h, k), rows.at[p, x, 1 - y, c, h, :, high], core)

    def third(h, k):
        p = planes[k]
        g_copy["xy", (h, k)].wait_recv()
        pass_on("xyc", (h, k), rows.at[p, :, 1 - y, c, h, :, low], core)
        g_copy["yx", (h, k)].wait_recv()
        pass_on("yxc", (h, k), rows.at[p, 1 - x, :, c, h, :, high], core)

    step = 512
    half_rows = 8 * slabs * half_tok

    def up_project(h, k):
        for kind in ("c", "xc", "yc", "xyc", "yxc"):
            g_copy[kind, (h, k)].wait_recv()
        p = planes[k]
        gain_cols = plane_cols(p)
        per = block // 2 // tok

        @pl.loop(0, 8)
        def _(b):
            @pl.loop(0, per)
            def _(s):
                spot = pl.ds(pl.multiple_of(s * tok, tok), tok)
                value = rows[p, b // 4, (b // 2) % 2, b % 2, h, spot, :].astype(F32)
                place = pl.ds(pl.multiple_of((b * per + s) * tok, tok), tok)
                square = squares[h, place, :]
                for i in range(plane // LANES):
                    strip = value[:, i * LANES : (i + 1) * LANES]
                    square = square + strip * strip
                squares[h, place, :] = square
                scaled[place, :] = (value * gain_ref[:, gain_cols]).astype(BF16)

        if h == 0:
            loads[k].wait()

        @pl.loop(0, ff2 // step)
        def _(n):
            columns = pl.ds(pl.multiple_of(n * step, step), step)
            got = jnp.dot(scaled[...], gate_up[k, :, columns], preferred_element_type=F32)
            if k:
                acc[h, :, columns] = acc[h, :, columns] + got
            else:
                acc[h, :, columns] = got

    me = g * 4 + t
    half_lane = lax.broadcasted_iota(jnp.int32, (half_tok, LANES), 1)
    picked = (half_lane == me) | (half_lane == me + experts)
    halves = slabs // 2
    quarters = [pl.ds(0, halves), pl.ds(halves, slabs - halves)]
    pair = [(2, 3), (0, 1)]

    def clear(h):
        own = pl.ds(pl.multiple_of(z * half_tok, half_tok), half_tok)
        for q in range(slabs):
            hidden[q, h * half_tok : (h + 1) * half_tok] = rows[q, x, y, c, h, own, :]
        for (kind, unit), copy in g_copy.items():
            if unit[0] == h:
                copy.wait_send()
        for copy in pending[g_start + h * (slabs - 1) : g_start + (h + 1) * (slabs - 1)]:
            copy.wait_send()

    def spots(k):
        return pl.ds(k * half_tok, half_tok)

    def both(u):
        return pl.ds(pair[u][0] * half_tok, 2 * half_tok)

    cut = 3 * plane // 8 // LANES * LANES
    part_a, part_d = pl.ds(0, cut), pl.ds(cut, plane - cut)
    c_copy, x_copy, y2_copy, d_copy = {}, {}, {}, {}
    zk = [take(2 * slabs) for _ in range(2)]

    def down_project(h, u):
        for cc in range(2):
            for i, k in enumerate(pair[u]):
                p = planes[k]
                for xx in range(2):
                    for yy in range(2):
                        source = c if cc == 0 else 1 - c
                        b = xx * 4 + yy * 2 + source
                        place = pl.ds(
                            pl.multiple_of((b * slabs + p) * half_tok, half_tok), half_tok
                        )
                        mean = jnp.sum(squares[h, place, :], axis=-1, keepdims=True)
                        scale = lax.rsqrt(mean * (1.0 / model) + 1e-06)
                        mine = gates[p, xx, yy, source, h * half_tok : (h + 1) * half_tok]
                        share = jnp.sum(
                            jnp.where(picked, mine.astype(F32), 0.0), axis=-1, keepdims=True
                        )
                        left = acc[h, place, :ff] * scale
                        right = acc[h, place, ff:] * (scale * share)
                        value = left / (1.0 + jnp.exp(-left)) * right
                        spot = (((cc * 2 + xx) * 2 + yy) * 2 + i) * half_tok
                        act[spot : spot + half_tok, :] = value.astype(BF16)
        if u == 0 and h == 0:
            loads[slabs].wait()
        tile = plane // 2
        for part_of in range(2):

            @pl.loop(part_of * slabs, (part_of + 1) * slabs)
            def _(n):
                got = jnp.dot(
                    act[...],
                    down[:, pl.ds(pl.multiple_of(n * tile, tile), tile)],
                    preferred_element_type=F32,
                ).astype(BF16)
                columns = pl.ds(pl.multiple_of((n % 2) * tile, tile), tile)
                for cc in range(2):
                    for xx in range(2):
                        for yy in range(2):
                            spot = ((cc * 2 + xx) * 2 + yy) * tok
                            rows[n // 2, xx, yy, 1 - cc, h, both(u), columns] = got[
                                spot : spot + tok
                            ]

            q = quarters[part_of]
            c_copy[h, u, part_of] = send(
                rows.at[q, :, :, 0, h, both(u)], got_core.at[q, :, :, h, both(u)], core
            )

    def add_into(ref, other):
        ref[...] = (ref[...].astype(F32) + other.astype(F32)).astype(BF16)

    def add_cores(h, u):
        for part_of in range(2):
            c_copy[h, u, part_of].wait_recv()
            q0 = quarters[part_of].start

            @pl.loop(q0, q0 + quarters[part_of].size)
            def _(q):
                for xx in range(2):
                    for yy in range(2):
                        add_into(
                            rows.at[q, xx, yy, 1, h, both(u)], got_core[q, xx, yy, h, both(u)]
                        )

            q = quarters[part_of]
            x_copy[h, u, part_of] = send(
                rows.at[q, 1 - x, :, 1, h, both(u), part_d], got_x.at[q, :, h, both(u)], over_x
            )
            y2_copy[h, u, part_of] = send(
                rows.at[q, :, 1 - y, 1, h, both(u), part_a], got_y2.at[q, :, h, both(u)], over_y
            )

    def send_home(h, k, src, landing, index):
        copy = copy_of(
            src, landing.at[z, h], zk[h] + index + k, zk[h] + index + z, device(planes[k], x, y, c)
        )
        copy.start()
        pending.append(copy)

    def add_second(h, u):
        for part_of in range(2):
            q0 = quarters[part_of].start
            x_copy[h, u, part_of].wait_recv()

            @pl.loop(q0, q0 + quarters[part_of].size)
            def _(q):
                for yy in range(2):
                    add_into(rows.at[q, x, yy, 1, h, both(u), part_d], got_x[q, yy, h, both(u)])

        d_copy[h, u] = send(
            rows.at[:, x, 1 - y, 1, h, both(u), part_d], last_d.at[:, h, both(u)], over_y
        )
        for part_of in range(2):
            q0 = quarters[part_of].start
            y2_copy[h, u, part_of].wait_recv()

            @pl.loop(q0, q0 + quarters[part_of].size)
            def _(q):
                for xx in range(2):
                    add_into(rows.at[q, xx, y, 1, h, both(u), part_a], got_y2[q, xx, h, both(u)])

        for k in pair[u]:
            if k:
                send_home(h, k, rows.at[:, :, y, 1, h, spots(k), part_a], landed_a, 0)

    def add_third(h, u):
        d_copy[h, u].wait_recv()

        @pl.loop(0, slabs)
        def _(q):
            add_into(rows.at[q, x, y, 1, h, both(u), part_d], last_d[q, h, both(u)])

        for k in pair[u]:
            if k:
                send_home(h, k, rows.at[:, x, y, 1, h, spots(k), part_d], landed_d, slabs)

    a_copy = {}

    def landed_sum(h):
        for p in others:
            copy_of(landed_a.at[p, h], landed_a.at[p, h], zk[h], zk[h] + p, core).wait_recv()

        @pl.loop(0, slabs)
        def _(q):
            for xx in range(2):
                total = rows[q, xx, y, 1, h, spots(0), part_a].astype(F32)
                for p in others:
                    total = total + landed_a[p, h, q, xx].astype(F32)
                rows[q, xx, y, 1, h, spots(0), part_a] = total.astype(BF16)

        a_copy[h] = send(rows.at[:, 1 - x, y, 1, h, spots(0), part_a], last_a.at[h], over_x)

    def output(h):
        place = slice(h * half_tok, (h + 1) * half_tok)
        for p in others:
            copy_of(
                landed_d.at[p, h], landed_d.at[p, h], zk[h], zk[h] + slabs + p, core
            ).wait_recv()
        for q in range(slabs):
            total = hidden[q, place, part_d].astype(F32)
            total = total + rows[q, x, y, 1, h, spots(0), part_d].astype(F32)
            for p in others:
                total = total + landed_d[p, h, q].astype(F32)
            out_ref[place, q * plane + cut : (q + 1) * plane] = total.astype(BF16)
        a_copy[h].wait_recv()
        for q in range(slabs):
            total = hidden[q, place, part_a].astype(F32)
            total = total + rows[q, x, y, 1, h, spots(0), part_a].astype(F32)
            total = total + last_a[h, q].astype(F32)
            out_ref[place, q * plane : q * plane + cut] = total.astype(BF16)

    first(0, 0)
    first(0, 1)
    second(0, 0)
    first(0, 2)
    gate_x.wait_recv()
    gate_y = send(gates.at[:, :, y, c], gates.at[:, :, y, c], over_y)
    second(0, 1)
    third(0, 0)
    first(0, 3)
    second(0, 2)
    gate_y.wait_recv()
    gate_c = send(gates.at[:, :, :, c], gates.at[:, :, :, c], core)
    up_project(0, 0)
    third(0, 1)
    first(1, 0)
    second(0, 3)
    up_project(0, 1)
    third(0, 2)
    first(1, 1)
    second(1, 0)
    up_project(0, 2)
    third(0, 3)
    first(1, 2)
    second(1, 1)
    third(1, 0)
    up_project(0, 3)
    clear(0)
    gate_c.wait_recv()
    first(1, 3)
    second(1, 2)
    down_project(0, 0)
    third(1, 1)
    add_cores(0, 0)
    second(1, 3)
    down_project(0, 1)
    third(1, 2)
    up_project(1, 0)
    add_cores(0, 1)
    third(1, 3)
    up_project(1, 1)
    add_second(0, 0)
    up_project(1, 2)
    add_third(0, 0)
    up_project(1, 3)
    clear(1)
    add_second(0, 1)
    down_project(1, 0)
    add_third(0, 1)
    add_cores(1, 0)
    down_project(1, 1)
    add_cores(1, 1)
    landed_sum(0)
    add_second(1, 0)
    output(0)
    add_third(1, 0)
    add_second(1, 1)
    landed_sum(1)
    add_third(1, 1)
    output(1)
    for copy in pending[:g_start] + pending[g_start + 2 * (slabs - 1) :]:
        if all(copy is not other for other in g_copy.values()):
            copy.wait_send()
    for i in range(chunks):
        chain_do(i, None, lambda copy: copy.wait_send())
        for p in others:
            chain_do(i, p, lambda copy: copy.wait_send())
    assert count[0] <= copies_max, count[0]


def layer(queries, keys, values, docs, out_proj, residual, gain, ids, weights, gate_up, down, groups):
    slabs = groups // 2
    tok, model = residual.shape
    tokens, depth = queries.shape
    plane = model // slabs
    ff, ff2 = down.shape[0], gate_up.shape[1]
    total = tok * slabs * 8
    half = slabs * tok // 2
    cut = 3 * plane // 8 // LANES * LANES
    copies_max = 240
    dma = pltpu.SemaphoreType.DMA
    vmem = pl.BlockSpec(memory_space=pltpu.VMEM)
    hbm = pl.BlockSpec(memory_space=pl.ANY)
    return pl.pallas_call(
        functools.partial(layer_kernel, slabs, copies_max),
        out_shape=jax.ShapeDtypeStruct((tok, model), BF16),
        in_specs=[hbm] * 3 + [vmem] + [hbm] * 2 + [vmem] * 3 + [hbm] * 2,
        out_specs=vmem,
        scratch_shapes=[
            pltpu.VMEM(queries.shape, BF16),
            pltpu.VMEM(keys.shape, BF16),
            pltpu.VMEM(values.shape, BF16),
            pltpu.VMEM(out_proj.shape, BF16),
            pltpu.VMEM(residual.shape, BF16),
            pltpu.VMEM((tokens, depth), BF16),
            pltpu.VMEM(out_proj.shape, BF16),
            pltpu.VMEM((slabs, tokens, depth), BF16),
            pltpu.VMEM((slabs, tok, plane), BF16),
            pltpu.VMEM((slabs, 2, 2, tok, plane), F32),
            pltpu.VMEM((slabs, 2, tok, plane), F32),
            pltpu.VMEM((slabs, tok, plane), BF16),
            pltpu.VMEM((slabs, tok, plane), BF16),
            pltpu.VMEM((slabs, 2, 2, 2, tok, LANES), BF16),
            pltpu.VMEM((slabs, 2, 2, 2, 2, half, plane), BF16),
            pltpu.VMEM((total // 2, plane), BF16),
            pltpu.VMEM((2, total // 2, LANES), F32),
            pltpu.VMEM((2, total // 2, ff2), F32),
            pltpu.VMEM((8 * tok, ff), BF16),
            pltpu.VMEM((slabs, plane, ff2), BF16),
            pltpu.VMEM((ff, model), BF16),
            pltpu.VMEM((slabs, tok, plane), BF16),
            pltpu.VMEM((slabs, 2, 2, 2, half, plane), BF16),
            pltpu.VMEM((slabs, 2, 2, half, plane - cut), BF16),
            pltpu.VMEM((slabs, 2, 2, half, cut), BF16),
            pltpu.VMEM((slabs, 2, half, plane - cut), BF16),
            pltpu.VMEM((2, slabs, tok // 2, cut), BF16),
            pltpu.VMEM((slabs, 2, slabs, 2, tok // 2, cut), BF16),
            pltpu.VMEM((slabs, 2, slabs, tok // 2, plane - cut), BF16),
            dma((slabs + 6,)),
            dma((copies_max,)),
            dma((copies_max,)),
        ],
        compiler_params=pltpu.CompilerParams(
            collective_id=0, has_side_effects=True, vmem_limit_bytes=VMEM_LIMIT
        ),
    )(queries, keys, values, docs, out_proj, residual, gain, ids, weights, gate_up, down)


def spread_gates(expert_ids, gate_weights, experts):
    gates = jnp.sum(
        jnp.where(
            expert_ids[:, :, None] == jnp.arange(experts, dtype=jnp.int32)[None, None, :],
            gate_weights[:, :, None],
            0.0,
        ),
        axis=1,
    )
    high = lax.reduce_precision(gates, 8, 7)
    low = gates - high
    pad = -(2 * experts) % LANES
    return jnp.concatenate(
        [high, low, jnp.zeros((gates.shape[0], pad), F32)], axis=1
    ).astype(BF16)


def plain_layer(head_out, out_proj, residual, gain, extra, gate_up, down, groups, tensors):
    experts = groups * tensors
    tok, model = residual.shape
    heads = lax.all_gather(head_out, "group", axis=0, tiled=True)
    part = jnp.dot(heads, out_proj, preferred_element_type=F32)
    part = part.reshape(groups, tensors, tok, part.shape[1])
    part = lax.psum_scatter(part, "tensor", scatter_dimension=1, tiled=False)
    attended = lax.all_to_all(part, "group", split_axis=0, concat_axis=2, tiled=True)
    hidden = residual.astype(F32) + attended.reshape(tok, model)
    mean_square = jnp.mean(hidden * hidden, axis=-1, keepdims=True)
    normed = (hidden * lax.rsqrt(mean_square + 1e-06) * gain).astype(BF16)
    rows = jnp.concatenate([normed, extra], axis=1)
    rows_all = lax.all_gather(rows, ("group", "tensor"), axis=0, tiled=True)
    me = lax.axis_index("group") * tensors + lax.axis_index("tensor")
    lane = jnp.arange(extra.shape[1], dtype=jnp.int32)
    picked = (lane == me) | (lane == me + experts)
    gate_col = jnp.sum(
        jnp.where(picked[None, :], rows_all[:, model:].astype(F32), 0.0), axis=1, keepdims=True
    )
    ff = down.shape[0]
    projected = jnp.dot(rows_all[:, :model], gate_up, preferred_element_type=F32)
    activated = (jax.nn.silu(projected[:, :ff]) * projected[:, ff:]).astype(BF16)
    expert_out = jnp.dot(activated, down, preferred_element_type=F32)
    weighted = (expert_out * gate_col).astype(BF16)
    expert_sum = lax.psum_scatter(weighted, ("group", "tensor"), scatter_dimension=0, tiled=True)
    return (hidden + expert_sum.astype(F32)).astype(BF16)


def on_device(
    queries,
    keys,
    values,
    document_index,
    out_proj,
    residual_in,
    norm_gain,
    expert_ids,
    gate_weights,
    w_gate_up,
    w_down,
):
    groups, tensors = lax.axis_size("group"), lax.axis_size("tensor")
    gain = norm_gain[None, :]
    if groups == 8 and tensors == 4:
        return layer(
            queries,
            keys,
            values,
            document_index,
            out_proj,
            residual_in,
            gain,
            expert_ids,
            gate_weights,
            w_gate_up[0],
            w_down[0],
            groups,
        )
    head_out = attention(queries, keys, values, document_index)
    extra = spread_gates(expert_ids, gate_weights, groups * tensors)
    return plain_layer(
        head_out, out_proj, residual_in, gain, extra, w_gate_up[0], w_down[0], groups, tensors
    )


def solution(mesh):
    in_specs = (
        P("group", "tensor"),
        P("group", "tensor"),
        P("group", "tensor"),
        P("group", None),
        P("tensor", "group"),
        P(("group", "tensor"), None),
        P(),
        P(("group", "tensor"), None),
        P(("group", "tensor"), None),
        P(("group", "tensor"), None, None),
        P(("group", "tensor"), None, None),
    )
    out_specs = P(("group", "tensor"), None)
    return jax.shard_map(
        on_device, mesh=mesh, in_specs=in_specs, out_specs=out_specs, check_vma=False
    )
```

```python
import functools

import jax
import jax.numpy as jnp
from jax import lax
from jax.experimental import pallas as pl
from jax.experimental.pallas import tpu as pltpu
from jax.sharding import PartitionSpec as P

HEAD_SIZE = 128
LANES = 128
MESH = pl.DeviceIdType.MESH
VMEM_LIMIT = 62 * 1024 * 1024
F32 = jnp.float32
BF16 = jnp.bfloat16


def attention(queries, keys, values, document_index):
    token_group = queries.shape[0]
    kv_dev = keys.shape[1] // HEAD_SIZE
    query_dev = queries.shape[1] // HEAD_SIZE
    group_ratio = query_dev // kv_dev
    query_head_split = queries.reshape(token_group, kv_dev, group_ratio, HEAD_SIZE)
    key_head_split = keys.reshape(token_group, kv_dev, HEAD_SIZE)
    value_head_split = values.reshape(token_group, kv_dev, HEAD_SIZE)
    scores = jnp.einsum(
        "qgrd,kgd->grqk", query_head_split, key_head_split, preferred_element_type=F32
    ) * (1.0 / HEAD_SIZE**0.5)
    doc_row = document_index[0]
    positions = jnp.arange(token_group, dtype=jnp.int32)
    visible = (positions[:, None] >= positions[None, :]) & (doc_row[:, None] == doc_row[None, :])
    scores = jnp.where(visible, scores, -jnp.inf)
    row_max = jnp.max(scores, axis=-1, keepdims=True)
    exponent = jnp.where(visible, jnp.exp(scores - row_max), 0.0)
    weights = (exponent / jnp.sum(exponent, axis=-1, keepdims=True)).astype(BF16)
    head_out = jnp.einsum("grqk,kgd->qgrd", weights, value_head_split, preferred_element_type=F32)
    return head_out.astype(BF16).reshape(token_group, query_dev * HEAD_SIZE)


def device(z, x, y, c):
    return (z * 2 + x, y * 2 + c)


def nearest_first(z):
    first = jnp.where(z == 0, 1, jnp.where(z == 1, 2, jnp.where(z == 2, 1, 2)))
    second = jnp.where(z == 0, 2, jnp.where(z == 1, 0, jnp.where(z == 2, 3, 1)))
    third = jnp.where(z <= 1, 3, 0)
    return [first, second, third]


def layer_kernel(
    slabs,
    copies_max,
    query_hbm,
    key_hbm,
    value_hbm,
    doc_ref,
    proj_hbm,
    res_hbm,
    gain_ref,
    ids_ref,
    weight_ref,
    gate_up_hbm,
    down_hbm,
    out_ref,
    query_ref,
    key_ref,
    value_ref,
    proj_ref,
    res_ref,
    head_own,
    proj_x,
    heads,
    res_in,
    part,
    got_half,
    sum_half,
    got_y,
    ids_pad,
    weight_pad,
    gates,
    rows,
    squares,
    acc,
    act,
    gate_up,
    down,
    hidden,
    got_core,
    got_x,
    got_y2,
    last_d,
    last_a,
    landed_a,
    landed_d,
    load_sem,
    send_sems,
    recv_sems,
):
    g, t = lax.axis_index("group"), lax.axis_index("tensor")
    z, x, y, c = g // 2, g % 2, t // 2, t % 2
    tok, model = res_ref.shape
    plane = model // slabs
    width = plane // 2
    ff2 = gate_up.shape[2]
    ff = ff2 // 2
    experts = slabs * 8
    block = slabs * tok
    others = nearest_first(z)
    planes = [z] + others
    core, over_y, over_x = device(z, x, y, 1 - c), device(z, x, 1 - y, c), device(z, 1 - x, y, c)

    def plane_cols(p):
        return pl.ds(pl.multiple_of(p * plane, plane), plane)

    small = [
        pltpu.make_async_copy(source, target, load_sem.at[slabs + 1 + i])
        for i, (source, target) in enumerate(
            [
                (key_hbm, key_ref),
                (query_hbm, query_ref),
                (value_hbm, value_ref),
                (proj_hbm, proj_ref),
                (res_hbm, res_ref),
            ]
        )
    ]
    for load in small:
        load.start()
    barrier = pltpu.get_barrier_semaphore()
    partners = [core, over_y, over_x] + [device(p, x, y, c) for p in others]
    for partner in partners:
        pl.semaphore_signal(barrier, inc=1, device_id=partner, device_id_type=MESH)
    loads = [
        pltpu.make_async_copy(
            gate_up_hbm.at[pl.ds(pl.multiple_of(planes[k] * plane, plane), plane)],
            gate_up.at[k],
            load_sem.at[k],
        )
        for k in range(slabs)
    ]
    loads.append(pltpu.make_async_copy(down_hbm, down, load_sem.at[slabs]))

    ids_pad[...] = jnp.zeros_like(ids_pad)
    weight_pad[...] = jnp.zeros_like(weight_pad)
    ids_pad[:, :tok] = ids_ref[...]
    weight_pad[:, :tok] = weight_ref[...]
    expert = lax.broadcasted_iota(jnp.int32, (LANES, LANES), 0)
    gate = jnp.zeros((LANES, LANES), F32)
    for k in range(ids_ref.shape[0]):
        chosen = ids_pad[k : k + 1, :]
        hit = (expert == chosen) | (expert == chosen + experts)
        gate = gate + jnp.where(hit, weight_pad[k : k + 1, :], 0.0)
    gate_high = gate.astype(BF16).astype(F32)
    gate = jnp.where(expert < experts, gate_high, gate - gate_high)
    gates[z, x, y, c] = gate.T[:tok].astype(BF16)
    squares[...] = jnp.zeros_like(squares)

    for load in small[:3]:
        load.wait()
    for load in loads:
        load.start()

    def attend():
        tokens = query_ref.shape[0]
        doc = jnp.broadcast_to(doc_ref[...].astype(F32), (tokens, tokens))
        row = lax.broadcasted_iota(jnp.int32, (tokens, tokens), 0)
        column = lax.broadcasted_iota(jnp.int32, (tokens, tokens), 1)
        visible = (row >= column) & (doc == doc.T)
        for h in range(query_ref.shape[1] // HEAD_SIZE):
            span = slice(h * HEAD_SIZE, (h + 1) * HEAD_SIZE)
            scores = lax.dot_general(
                query_ref[:, span],
                key_ref[...],
                (((1,), (1,)), ((), ())),
                preferred_element_type=F32,
            ) * (1.0 / HEAD_SIZE**0.5)
            scores = jnp.where(visible, scores, -jnp.inf)
            exponent = jnp.exp(scores - jnp.max(scores, axis=-1, keepdims=True))
            total = jnp.sum(exponent, axis=-1, keepdims=True)
            probs = (exponent / total).astype(BF16)
            head_own[:, span] = jnp.dot(
                probs, value_ref[...], preferred_element_type=F32
            ).astype(BF16)

    attend()
    for load in small[3:]:
        load.wait()
    pl.semaphore_wait(barrier, len(partners))

    count = [0]
    pending = []

    def copy_of(src, dst, send_index, recv_index, target):
        return pltpu.make_async_remote_copy(
            src_ref=src,
            dst_ref=dst,
            send_sem=send_sems.at[send_index],
            recv_sem=recv_sems.at[recv_index],
            device_id=target,
            device_id_type=MESH,
        )

    def take(n):
        k = count[0]
        count[0] = k + n
        return k

    def send(src, dst, target):
        k = take(1)
        copy = copy_of(src, dst, k, k, target)
        copy.start()
        pending.append(copy)
        return copy

    def send_planes(source, target):
        k = take(slabs)
        for i, p in enumerate(others):
            copy = copy_of(source(p), target(z), k + i, k + z, device(p, x, y, c))
            copy.start()
            pending.append(copy)
        return lambda p: copy_of(target(p), target(p), k, k + p, core)

    pieces = [(0, width // 2), (width // 2, width // 4), (3 * width // 4, width // 4)]
    proj_copy = []
    for start, size in pieces:
        cols = pl.ds(start, size)
        proj_copy.append(send(proj_ref.at[:, cols], proj_x.at[:, cols], over_x))
    above = device(jnp.minimum(z + 1, slabs - 1), x, y, c)
    below = device(jnp.maximum(z - 1, 0), x, y, c)
    is_low, is_high = z < slabs - 1, z > 0
    chunks = 2
    chunk = head_own.shape[1] // chunks
    chain = [take(slabs + 2) for _ in range(chunks)]
    spans = [pl.ds(i * chunk, chunk) for i in range(chunks)]

    def own_copy(i, rising):
        return copy_of(
            head_own.at[:, spans[i]],
            heads.at[z, :, spans[i]],
            chain[i] + slabs + (0 if rising else 1),
            chain[i] + z,
            above if rising else below,
        )

    def relay_copy(i, p, target):
        spot = heads.at[p, :, spans[i]]
        return copy_of(spot, spot, chain[i] + p, chain[i] + p, target)

    def chain_do(i, p, act_on):
        if p is None:
            rising, falling = is_low, is_high
        else:
            rising, falling = (p < z) & is_low, (p > z) & is_high

        @pl.when(rising)
        def _():
            act_on(own_copy(i, True) if p is None else relay_copy(i, p, above))

        @pl.when(falling)
        def _():
            act_on(own_copy(i, False) if p is None else relay_copy(i, p, below))

    for i in range(chunks):
        chain_do(i, None, lambda copy: copy.start())

    def relay(p):
        for i in range(chunks):
            relay_copy(i, p, above).wait_recv()
            chain_do(i, p, lambda copy: copy.start())

    def project(k, weights, columns):
        source = head_own[...] if k == 0 else heads[planes[k]]
        got = jnp.dot(source, weights, preferred_element_type=F32)
        for yy in range(2):
            for cc in range(2):
                start = (yy * 2 + cc) * tok
                part[k, cc, yy, :, columns] = got[start : start + tok]

    def columns_of(i):
        if i == 0:
            return pl.ds(pl.multiple_of(x * width, width), width)
        start, size = pieces[i - 1]
        return pl.ds(pl.multiple_of((1 - x) * width + start, LANES), size)

    half_copy, y_copy = {}, {}

    def to_core(i, ks):
        columns = columns_of(i)
        half_copy[i, ks] = send(
            part.at[pl.ds(ks[0], len(ks)), 1 - c, :, :, columns],
            got_half.at[pl.ds(ks[0], len(ks)), :, :, columns],
            core,
        )

    def over_cores(i, ks):
        columns = columns_of(i)
        half_copy[i, ks].wait_recv()
        for k in ks:
            total = part[k, c, 1 - y, :, columns] + got_half[k, 1 - y, :, columns]
            sum_half[k, :, columns] = total.astype(BF16)
        spot = pl.ds(ks[0], len(ks))
        y_copy[i, ks] = send(
            sum_half.at[spot, :, columns], got_y.at[spot, :, columns], over_y
        )
        for k in ks:
            part[k, c, y, :, columns] = part[k, c, y, :, columns] + got_half[k, y, :, columns]

    half_tok = tok // 2

    def finish(i, ks):
        columns = columns_of(i)
        y_copy[i, ks].wait_recv()
        for k in ks:
            total = part[k, c, y, :, columns] + got_y[k, :, columns].astype(F32)
            total = (total + res_in[planes[k], :, columns].astype(F32)).astype(BF16)
            spot = pl.ds(pl.multiple_of(planes[k] * half_tok, half_tok), half_tok)
            for h in range(2):
                rows[z, x, y, c, h, spot, columns] = total[h * half_tok : (h + 1) * half_tok]

    def fold(k):
        loads[k].wait()

        @pl.loop(0, plane // LANES)
        def _(r):
            start = pl.multiple_of(planes[k] * plane + r * LANES, LANES)
            scale = jnp.broadcast_to(gain_ref[:, pl.ds(start, LANES)], (LANES, LANES)).T
            spot = pl.ds(pl.multiple_of(r * LANES, LANES), LANES)
            for n in range(ff2 // LANES):
                columns = slice(n * LANES, (n + 1) * LANES)
                value = gate_up[k, spot, columns].astype(F32) * scale
                gate_up[k, spot, columns] = value.astype(BF16)

    every = tuple(range(slabs))
    project(0, proj_ref[...], columns_of(0))
    to_core(0, (0,))
    fold(0)
    fold(1)
    relay(planes[1])
    relay(planes[2])
    res_wait = send_planes(lambda p: res_ref.at[:, plane_cols(p)], lambda p: res_in.at[p])
    gate_wait = send_planes(lambda p: gates.at[z, x, y, c], lambda p: gates.at[p, x, y, c])
    for k in (1, 2):
        project(k, proj_ref[...], columns_of(0))
        to_core(0, (k,))
    fold(2)
    fold(3)
    relay(planes[3])
    project(3, proj_ref[...], columns_of(0))
    to_core(0, (3,))
    for k in range(slabs):
        over_cores(0, (k,))
    for i, (start, size) in enumerate(pieces):
        proj_copy[i].wait_recv()
        for k in range(slabs):
            project(k, proj_x[:, start : start + size], columns_of(1 + i))
        to_core(1 + i, every)
        if i == 0:
            res_in[z] = res_ref[:, plane_cols(z)]
        over_cores(1 + i, every)
    for p in others:
        res_wait(p).wait_recv()
    for k in range(slabs):
        finish(0, (k,))
    for i in range(len(pieces)):
        finish(1 + i, every)

    low, high = pl.ds(0, width), pl.ds(width, width)
    g_copy = {}

    def pass_on(kind, unit, spot, target):
        g_copy[kind, unit] = send(spot, spot, target)

    z_wait = {}

    def send_half(h):
        before = len(pending)
        z_wait[h] = send_planes(
            lambda p: rows.at[z, x, y, c, h], lambda p: rows.at[p, x, y, c, h]
        )
        for i, copy in enumerate(pending[before:]):
            g_copy["z", (h, i)] = copy

    for p in others:
        gate_wait(p).wait_recv()
    gate_x = send(gates.at[:, x, y, c], gates.at[:, x, y, c], over_x)
    gate_copy = {}

    def gates_y():
        gate_x.wait_recv()
        gate_copy["y"] = send(gates.at[:, :, y, c], gates.at[:, :, y, c], over_y)

    def gates_c():
        gate_copy["y"].wait_recv()
        gate_copy["c"] = send(gates.at[:, :, :, c], gates.at[:, :, :, c], core)

    def gates_done():
        gate_copy["c"].wait_recv()

    def first(h, k):
        p = planes[k]
        if k:
            z_wait[h](p).wait_recv()
        pass_on("x", (h, k), rows.at[p, x, y, c, h, :, low], over_x)
        pass_on("y", (h, k), rows.at[p, x, y, c, h, :, high], over_y)
        pass_on("c", (h, k), rows.at[p, x, y, c, h], core)

    def second_x(h, k):
        p = planes[k]
        g_copy["x", (h, k)].wait_recv()
        pass_on("xy", (h, k), rows.at[p, :, y, c, h, :, low], over_y)
        pass_on("xc", (h, k), rows.at[p, 1 - x, y, c, h, :, low], core)

    def second_y(h, k):
        p = planes[k]
        g_copy["y", (h, k)].wait_recv()
        pass_on("yx", (h, k), rows.at[p, x, :, c, h, :, high], over_x)
        pass_on("yc", (h, k), rows.at[p, x, 1 - y, c, h, :, high], core)

    def third_x(h, k):
        p = planes[k]
        g_copy["xy", (h, k)].wait_recv()
        pass_on("xyc", (h, k), rows.at[p, :, 1 - y, c, h, :, low], core)

    def third_y(h, k):
        p = planes[k]
        g_copy["yx", (h, k)].wait_recv()
        pass_on("yxc", (h, k), rows.at[p, 1 - x, :, c, h, :, high], core)

    step = 512
    half_rows = 8 * slabs * half_tok

    def up_project(h, k):
        for kind in ("c", "xc", "yc", "xyc", "yxc"):
            g_copy[kind, (h, k)].wait_recv()
        p = planes[k]
        per = block // 2 // tok

        @pl.loop(0, 8)
        def _(b):
            for s in range(per):
                spot = pl.ds(s * tok, tok)
                value = rows[p, b // 4, (b // 2) % 2, b % 2, h, spot, :].astype(F32)
                place = pl.ds(pl.multiple_of((b * per + s) * tok, tok), tok)
                square = squares[h, place, :]
                for i in range(plane // LANES):
                    strip = value[:, i * LANES : (i + 1) * LANES]
                    square = square + strip * strip
                squares[h, place, :] = square

        @pl.loop(0, ff2 // step)
        def _(n):
            columns = pl.ds(pl.multiple_of(n * step, step), step)
            tokens = rows[p, :, :, :, h].reshape(half_rows, plane)
            got = jnp.dot(tokens, gate_up[k, :, columns], preferred_element_type=F32)
            if k:
                acc[h, :, columns] = acc[h, :, columns] + got
            else:
                acc[h, :, columns] = got

    me = g * 4 + t
    half_lane = lax.broadcasted_iota(jnp.int32, (half_tok, LANES), 1)
    picked = (half_lane == me) | (half_lane == me + experts)

    def clear(h):
        own = pl.ds(pl.multiple_of(z * half_tok, half_tok), half_tok)
        for q in range(slabs):
            hidden[q, h * half_tok : (h + 1) * half_tok] = rows[q, x, y, c, h, own, :]
        for (kind, unit), copy in g_copy.items():
            if unit[0] == h:
                copy.wait_send()

    def spots(k):
        return pl.ds(k * half_tok, half_tok)

    cut = 3 * plane // 8 // LANES * LANES
    part_a, part_d = pl.ds(0, cut), pl.ds(cut, plane - cut)
    c_copy, x_copy, y2_copy, d_copy, a_copy = {}, {}, {}, {}, {}
    zk = {(h, q): take(2 * slabs) for h in range(2) for q in range(slabs)}
    chunk_rows = slabs * half_tok

    def down_act(h):
        for cc in range(2):
            for k in range(slabs):
                p = planes[k]
                for xx in range(2):
                    for yy in range(2):
                        source = c if cc == 0 else 1 - c
                        b = xx * 4 + yy * 2 + source
                        place = pl.ds(
                            pl.multiple_of((b * slabs + p) * half_tok, half_tok), half_tok
                        )
                        mean = jnp.sum(squares[h, place, :], axis=-1, keepdims=True)
                        scale = lax.rsqrt(mean * (1.0 / model) + 1e-06)
                        mine = gates[p, xx, yy, source, h * half_tok : (h + 1) * half_tok]
                        share = jnp.sum(
                            jnp.where(picked, mine.astype(F32), 0.0), axis=-1, keepdims=True
                        )
                        left = acc[h, place, :ff] * scale
                        right = acc[h, place, ff:] * (scale * share)
                        value = left / (1.0 + jnp.exp(-left)) * right
                        spot = ((cc * 2 + xx) * 2 + yy) * chunk_rows + k * half_tok
                        act[spot : spot + half_tok, :] = value.astype(BF16)
        if h == 0:
            loads[slabs].wait()

    def down_project(h, q):
        tile = plane // 2

        @pl.loop(2 * q, 2 * q + 2)
        def _(n):
            got = jnp.dot(
                act[...],
                down[:, pl.ds(pl.multiple_of(n * tile, tile), tile)],
                preferred_element_type=F32,
            ).astype(BF16)
            columns = pl.ds(pl.multiple_of((n % 2) * tile, tile), tile)
            for cc in range(2):
                for xx in range(2):
                    for yy in range(2):
                        spot = ((cc * 2 + xx) * 2 + yy) * chunk_rows
                        rows[q, xx, yy, 1 - cc, h, :, columns] = got[spot : spot + chunk_rows]

        c_copy[h, q] = send(rows.at[q, :, :, 0, h], got_core.at[q, :, :, h], core)

    def add_into(ref, other):
        count_rows = ref.shape[0]
        for start in range(0, count_rows, 32):
            spot = slice(start, start + 32)
            ref[spot, :] = (ref[spot, :].astype(F32) + other[spot, :].astype(F32)).astype(BF16)

    def add_cores(h, q):
        c_copy[h, q].wait_recv()
        for xx in range(2):
            for yy in range(2):
                add_into(rows.at[q, xx, yy, 1, h], got_core.at[q, xx, yy, h])
        x_copy[h, q] = send(rows.at[q, 1 - x, :, 1, h, :, part_d], got_x.at[q, :, h], over_x)
        y2_copy[h, q] = send(rows.at[q, :, 1 - y, 1, h, :, part_a], got_y2.at[q, :, h], over_y)

    def send_home(h, q, source, landing, index):
        for k in range(1, slabs):
            copy = copy_of(
                source(k),
                landing.at[z, h, q],
                zk[h, q] + index + k,
                zk[h, q] + index + z,
                device(planes[k], x, y, c),
            )
            copy.start()
            pending.append(copy)

    def landed(h, q, landing, index):
        for p in others:
            spot = landing.at[p, h, q]
            copy_of(spot, spot, zk[h, q], zk[h, q] + index + p, core).wait_recv()

    def add_a(h, q):
        y2_copy[h, q].wait_recv()
        for xx in range(2):
            add_into(rows.at[q, xx, y, 1, h, :, part_a], got_y2.at[q, xx, h])
        send_home(h, q, lambda k: rows.at[q, :, y, 1, h, spots(k), part_a], landed_a, 0)

    def add_d(h, q):
        x_copy[h, q].wait_recv()
        for yy in range(2):
            add_into(rows.at[q, x, yy, 1, h, :, part_d], got_x.at[q, yy, h])
        d_copy[h, q] = send(rows.at[q, x, 1 - y, 1, h, :, part_d], last_d.at[q, h], over_y)

    def add_last(h, q):
        d_copy[h, q].wait_recv()
        add_into(rows.at[q, x, y, 1, h, :, part_d], last_d.at[q, h])
        send_home(h, q, lambda k: rows.at[q, x, y, 1, h, spots(k), part_d], landed_d, slabs)

    def landed_sum(h, q):
        landed(h, q, landed_a, 0)
        for xx in range(2):
            total = rows[q, xx, y, 1, h, spots(0), part_a].astype(F32)
            for p in others:
                total = total + landed_a[p, h, q, xx].astype(F32)
            rows[q, xx, y, 1, h, spots(0), part_a] = total.astype(BF16)
        a_copy[h, q] = send(
            rows.at[q, 1 - x, y, 1, h, spots(0), part_a], last_a.at[h, q], over_x
        )

    def output(h, q):
        place = slice(h * half_tok, (h + 1) * half_tok)
        landed(h, q, landed_d, slabs)
        total = hidden[q, place, part_d].astype(F32)
        total = total + rows[q, x, y, 1, h, spots(0), part_d].astype(F32)
        for p in others:
            total = total + landed_d[p, h, q].astype(F32)
        out_ref[place, q * plane + cut : (q + 1) * plane] = total.astype(BF16)
        a_copy[h, q].wait_recv()
        total = hidden[q, place, part_a].astype(F32)
        total = total + rows[q, x, y, 1, h, spots(0), part_a].astype(F32)
        total = total + last_a[h, q].astype(F32)
        out_ref[place, q * plane : q * plane + cut] = total.astype(BF16)

    send_half(0)
    first(0, 0)
    first(1, 0)
    second_y(0, 0)
    second_x(0, 0)
    second_x(1, 0)
    second_y(1, 0)
    first(0, 1)
    send_half(1)
    third_y(0, 0)
    third_x(0, 0)
    gates_y()
    up_project(0, 0)
    first(0, 2)
    third_y(1, 0)
    third_x(1, 0)
    second_x(0, 1)
    second_y(0, 1)
    first(0, 3)
    gates_c()
    up_project(1, 0)
    second_y(0, 2)
    second_x(0, 2)
    first(1, 1)
    third_y(0, 1)
    third_x(0, 1)
    second_y(0, 3)
    second_x(0, 3)
    up_project(0, 1)
    first(1, 2)
    third_y(0, 2)
    third_x(0, 2)
    second_y(1, 1)
    second_x(1, 1)
    up_project(0, 2)
    first(1, 3)
    third_y(0, 3)
    third_x(0, 3)
    second_y(1, 2)
    second_x(1, 2)
    up_project(0, 3)
    gates_done()
    clear(0)
    down_act(0)
    third_x(1, 1)
    third_y(1, 1)
    down_project(0, 0)
    second_x(1, 3)
    second_y(1, 3)
    down_project(0, 1)
    down_project(0, 2)
    third_x(1, 2)
    third_y(1, 2)
    add_cores(0, 0)
    down_project(0, 3)
    add_cores(0, 1)
    up_project(1, 1)
    third_y(1, 3)
    third_x(1, 3)
    add_cores(0, 2)
    add_cores(0, 3)
    up_project(1, 2)
    add_a(0, 0)
    add_d(0, 0)
    add_a(0, 1)
    up_project(1, 3)
    add_a(0, 2)
    clear(1)
    down_act(1)
    add_d(0, 1)
    down_project(1, 0)
    add_a(0, 3)
    landed_sum(0, 0)
    down_project(1, 1)
    add_last(0, 0)
    down_project(1, 2)
    add_d(0, 2)
    add_cores(1, 0)
    landed_sum(0, 1)
    add_last(0, 1)
    down_project(1, 3)
    add_cores(1, 1)
    landed_sum(0, 2)
    add_cores(1, 2)
    add_d(0, 3)
    landed_sum(0, 3)
    add_cores(1, 3)
    add_last(0, 2)
    output(0, 0)
    add_a(1, 0)
    add_d(1, 0)
    output(0, 1)
    add_a(1, 1)
    add_a(1, 2)
    add_d(1, 1)
    output(0, 2)
    landed_sum(1, 0)
    add_last(0, 3)
    landed_sum(1, 1)
    add_d(1, 2)
    add_a(1, 3)
    landed_sum(1, 2)
    add_last(1, 0)
    output(0, 3)
    add_last(1, 1)
    add_d(1, 3)
    landed_sum(1, 3)
    add_last(1, 2)
    output(1, 0)
    add_last(1, 3)
    output(1, 1)
    output(1, 2)
    output(1, 3)
    gathered = list(g_copy.values())
    for copy in pending:
        if all(copy is not other for other in gathered):
            copy.wait_send()
    for i in range(chunks):
        chain_do(i, None, lambda copy: copy.wait_send())
        for p in others:
            chain_do(i, p, lambda copy: copy.wait_send())
    assert count[0] <= copies_max, count[0]


def layer(queries, keys, values, docs, out_proj, residual, gain, ids, weights, gate_up, down, groups):
    slabs = groups // 2
    tok, model = residual.shape
    tokens, depth = queries.shape
    plane = model // slabs
    ff, ff2 = down.shape[0], gate_up.shape[1]
    total = tok * slabs * 8
    half = slabs * tok // 2
    cut = 3 * plane // 8 // LANES * LANES
    copies_max = 300
    dma = pltpu.SemaphoreType.DMA
    vmem = pl.BlockSpec(memory_space=pltpu.VMEM)
    hbm = pl.BlockSpec(memory_space=pl.ANY)
    return pl.pallas_call(
        functools.partial(layer_kernel, slabs, copies_max),
        out_shape=jax.ShapeDtypeStruct((tok, model), BF16),
        in_specs=[hbm] * 3 + [vmem] + [hbm] * 2 + [vmem] * 3 + [hbm] * 2,
        out_specs=vmem,
        scratch_shapes=[
            pltpu.VMEM(queries.shape, BF16),
            pltpu.VMEM(keys.shape, BF16),
            pltpu.VMEM(values.shape, BF16),
            pltpu.VMEM(out_proj.shape, BF16),
            pltpu.VMEM(residual.shape, BF16),
            pltpu.VMEM((tokens, depth), BF16),
            pltpu.VMEM(out_proj.shape, BF16),
            pltpu.VMEM((slabs, tokens, depth), BF16),
            pltpu.VMEM((slabs, tok, plane), BF16),
            pltpu.VMEM((slabs, 2, 2, tok, plane), F32),
            pltpu.VMEM((slabs, 2, tok, plane), F32),
            pltpu.VMEM((slabs, tok, plane), BF16),
            pltpu.VMEM((slabs, tok, plane), BF16),
            pltpu.VMEM((ids.shape[0], LANES), jnp.int32),
            pltpu.VMEM((ids.shape[0], LANES), F32),
            pltpu.VMEM((slabs, 2, 2, 2, tok, LANES), BF16),
            pltpu.VMEM((slabs, 2, 2, 2, 2, half, plane), BF16),
            pltpu.VMEM((2, total // 2, LANES), F32),
            pltpu.VMEM((2, total // 2, ff2), F32),
            pltpu.VMEM((total // 2, ff), BF16),
            pltpu.VMEM((slabs, plane, ff2), BF16),
            pltpu.VMEM((ff, model), BF16),
            pltpu.VMEM((slabs, tok, plane), BF16),
            pltpu.VMEM((slabs, 2, 2, 2, half, plane), BF16),
            pltpu.VMEM((slabs, 2, 2, half, plane - cut), BF16),
            pltpu.VMEM((slabs, 2, 2, half, cut), BF16),
            pltpu.VMEM((slabs, 2, half, plane - cut), BF16),
            pltpu.VMEM((2, slabs, tok // 2, cut), BF16),
            pltpu.VMEM((slabs, 2, slabs, 2, tok // 2, cut), BF16),
            pltpu.VMEM((slabs, 2, slabs, tok // 2, plane - cut), BF16),
            dma((slabs + 6,)),
            dma((copies_max,)),
            dma((copies_max,)),
        ],
        compiler_params=pltpu.CompilerParams(
            collective_id=0, has_side_effects=True, vmem_limit_bytes=VMEM_LIMIT
        ),
    )(queries, keys, values, docs, out_proj, residual, gain, ids, weights, gate_up, down)


def spread_gates(expert_ids, gate_weights, experts):
    gates = jnp.sum(
        jnp.where(
            expert_ids[:, :, None] == jnp.arange(experts, dtype=jnp.int32)[None, None, :],
            gate_weights[:, :, None],
            0.0,
        ),
        axis=1,
    )
    high = lax.reduce_precision(gates, 8, 7)
    low = gates - high
    pad = -(2 * experts) % LANES
    return jnp.concatenate(
        [high, low, jnp.zeros((gates.shape[0], pad), F32)], axis=1
    ).astype(BF16)


def plain_layer(head_out, out_proj, residual, gain, extra, gate_up, down, groups, tensors):
    experts = groups * tensors
    tok, model = residual.shape
    heads = lax.all_gather(head_out, "group", axis=0, tiled=True)
    part = jnp.dot(heads, out_proj, preferred_element_type=F32)
    part = part.reshape(groups, tensors, tok, part.shape[1])
    part = lax.psum_scatter(part, "tensor", scatter_dimension=1, tiled=False)
    attended = lax.all_to_all(part, "group", split_axis=0, concat_axis=2, tiled=True)
    hidden = residual.astype(F32) + attended.reshape(tok, model)
    mean_square = jnp.mean(hidden * hidden, axis=-1, keepdims=True)
    normed = (hidden * lax.rsqrt(mean_square + 1e-06) * gain).astype(BF16)
    rows = jnp.concatenate([normed, extra], axis=1)
    rows_all = lax.all_gather(rows, ("group", "tensor"), axis=0, tiled=True)
    me = lax.axis_index("group") * tensors + lax.axis_index("tensor")
    lane = jnp.arange(extra.shape[1], dtype=jnp.int32)
    picked = (lane == me) | (lane == me + experts)
    gate_col = jnp.sum(
        jnp.where(picked[None, :], rows_all[:, model:].astype(F32), 0.0), axis=1, keepdims=True
    )
    ff = down.shape[0]
    projected = jnp.dot(rows_all[:, :model], gate_up, preferred_element_type=F32)
    activated = (jax.nn.silu(projected[:, :ff]) * projected[:, ff:]).astype(BF16)
    expert_out = jnp.dot(activated, down, preferred_element_type=F32)
    weighted = (expert_out * gate_col).astype(BF16)
    expert_sum = lax.psum_scatter(weighted, ("group", "tensor"), scatter_dimension=0, tiled=True)
    return (hidden + expert_sum.astype(F32)).astype(BF16)


def on_device(
    queries,
    keys,
    values,
    document_index,
    out_proj,
    residual_in,
    norm_gain,
    expert_ids,
    gate_weights,
    w_gate_up,
    w_down,
):
    groups, tensors = lax.axis_size("group"), lax.axis_size("tensor")
    gain = norm_gain[None, :]
    if groups == 8 and tensors == 4:
        return layer(
            queries,
            keys,
            values,
            document_index,
            out_proj,
            residual_in,
            gain,
            expert_ids.T,
            gate_weights.T,
            w_gate_up[0],
            w_down[0],
            groups,
        )
    head_out = attention(queries, keys, values, document_index)
    extra = spread_gates(expert_ids, gate_weights, groups * tensors)
    return plain_layer(
        head_out, out_proj, residual_in, gain, extra, w_gate_up[0], w_down[0], groups, tensors
    )


def solution(mesh):
    in_specs = (
        P("group", "tensor"),
        P("group", "tensor"),
        P("group", "tensor"),
        P("group", None),
        P("tensor", "group"),
        P(("group", "tensor"), None),
        P(),
        P(("group", "tensor"), None),
        P(("group", "tensor"), None),
        P(("group", "tensor"), None, None),
        P(("group", "tensor"), None, None),
    )
    out_specs = P(("group", "tensor"), None)
    return jax.shard_map(
        on_device, mesh=mesh, in_specs=in_specs, out_specs=out_specs, check_vma=False
    )
```

```python
import functools

import jax
import jax.numpy as jnp
from jax import lax
from jax.experimental import pallas as pl
from jax.experimental.pallas import tpu as pltpu
from jax.sharding import PartitionSpec as P

HEAD_SIZE = 128
LANES = 128
MESH = pl.DeviceIdType.MESH
VMEM_LIMIT = 62 * 1024 * 1024
F32 = jnp.float32
BF16 = jnp.bfloat16


def attention(queries, keys, values, document_index):
    token_group = queries.shape[0]
    kv_dev = keys.shape[1] // HEAD_SIZE
    query_dev = queries.shape[1] // HEAD_SIZE
    group_ratio = query_dev // kv_dev
    query_head_split = queries.reshape(token_group, kv_dev, group_ratio, HEAD_SIZE)
    key_head_split = keys.reshape(token_group, kv_dev, HEAD_SIZE)
    value_head_split = values.reshape(token_group, kv_dev, HEAD_SIZE)
    scores = jnp.einsum(
        "qgrd,kgd->grqk", query_head_split, key_head_split, preferred_element_type=F32
    ) * (1.0 / HEAD_SIZE**0.5)
    doc_row = document_index[0]
    positions = jnp.arange(token_group, dtype=jnp.int32)
    visible = (positions[:, None] >= positions[None, :]) & (doc_row[:, None] == doc_row[None, :])
    scores = jnp.where(visible, scores, -jnp.inf)
    row_max = jnp.max(scores, axis=-1, keepdims=True)
    exponent = jnp.where(visible, jnp.exp(scores - row_max), 0.0)
    weights = (exponent / jnp.sum(exponent, axis=-1, keepdims=True)).astype(BF16)
    head_out = jnp.einsum("grqk,kgd->qgrd", weights, value_head_split, preferred_element_type=F32)
    return head_out.astype(BF16).reshape(token_group, query_dev * HEAD_SIZE)


def device(z, x, y, c):
    return (z * 2 + x, y * 2 + c)


def nearest_first(z):
    first = jnp.where(z == 0, 1, jnp.where(z == 1, 2, jnp.where(z == 2, 1, 2)))
    second = jnp.where(z == 0, 2, jnp.where(z == 1, 0, jnp.where(z == 2, 3, 1)))
    third = jnp.where(z <= 1, 3, 0)
    return [first, second, third]


def layer_kernel(
    slabs,
    copies_max,
    send_slots,
    query_hbm,
    key_hbm,
    value_hbm,
    doc_ref,
    proj_hbm,
    res_hbm,
    gain_ref,
    ids_ref,
    weight_ref,
    gate_up_hbm,
    down_hbm,
    out_ref,
    query_ref,
    key_ref,
    value_ref,
    proj_ref,
    res_ref,
    head_own,
    proj_x,
    heads,
    res_in,
    part,
    got_half,
    sum_half,
    got_y,
    ids_pad,
    weight_pad,
    gates,
    rows,
    squares,
    acc,
    act,
    gate_up,
    down,
    hidden,
    got_core,
    got_x,
    got_y2,
    last_d,
    last_a,
    landed_a,
    landed_d,
    load_sem,
    send_sems,
    recv_sems,
):
    g, t = lax.axis_index("group"), lax.axis_index("tensor")
    z, x, y, c = g // 2, g % 2, t // 2, t % 2
    tok, model = res_ref.shape
    plane = model // slabs
    width = plane // 2
    ff2 = gate_up.shape[2]
    ff = ff2 // 2
    experts = slabs * 8
    block = slabs * tok
    others = nearest_first(z)
    planes = [z] + others
    core, over_y, over_x = device(z, x, y, 1 - c), device(z, x, 1 - y, c), device(z, 1 - x, y, c)

    def plane_cols(p):
        return pl.ds(pl.multiple_of(p * plane, plane), plane)

    small = [
        pltpu.make_async_copy(source, target, load_sem.at[slabs + 1 + i])
        for i, (source, target) in enumerate(
            [
                (key_hbm, key_ref),
                (query_hbm, query_ref),
                (value_hbm, value_ref),
                (proj_hbm, proj_ref),
                (res_hbm, res_ref),
            ]
        )
    ]
    for load in small:
        load.start()
    barrier = pltpu.get_barrier_semaphore()
    partners = [core, over_y, over_x] + [device(p, x, y, c) for p in others]
    for partner in partners:
        pl.semaphore_signal(barrier, inc=1, device_id=partner, device_id_type=MESH)
    loads = [
        pltpu.make_async_copy(
            gate_up_hbm.at[pl.ds(pl.multiple_of(planes[k] * plane, plane), plane)],
            gate_up.at[k],
            load_sem.at[k],
        )
        for k in range(slabs)
    ]
    loads.append(pltpu.make_async_copy(down_hbm, down, load_sem.at[slabs]))

    ids_pad[...] = jnp.zeros_like(ids_pad)
    weight_pad[...] = jnp.zeros_like(weight_pad)
    ids_pad[:, :tok] = ids_ref[...]
    weight_pad[:, :tok] = weight_ref[...]
    expert = lax.broadcasted_iota(jnp.int32, (LANES, LANES), 0)
    gate = jnp.zeros((LANES, LANES), F32)
    for k in range(ids_ref.shape[0]):
        chosen = ids_pad[k : k + 1, :]
        hit = (expert == chosen) | (expert == chosen + experts)
        gate = gate + jnp.where(hit, weight_pad[k : k + 1, :], 0.0)
    gate_high = gate.astype(BF16).astype(F32)
    gate = jnp.where(expert < experts, gate_high, gate - gate_high)
    gates[z, x, y, c] = gate.T[:tok].astype(BF16)
    squares[...] = jnp.zeros_like(squares)

    for load in small[:3]:
        load.wait()
    for load in loads:
        load.start()

    def attend():
        tokens = query_ref.shape[0]
        doc = jnp.broadcast_to(doc_ref[...].astype(F32), (tokens, tokens))
        row = lax.broadcasted_iota(jnp.int32, (tokens, tokens), 0)
        column = lax.broadcasted_iota(jnp.int32, (tokens, tokens), 1)
        visible = (row >= column) & (doc == doc.T)
        for h in range(query_ref.shape[1] // HEAD_SIZE):
            span = slice(h * HEAD_SIZE, (h + 1) * HEAD_SIZE)
            scores = lax.dot_general(
                query_ref[:, span],
                key_ref[...],
                (((1,), (1,)), ((), ())),
                preferred_element_type=F32,
            ) * (1.0 / HEAD_SIZE**0.5)
            scores = jnp.where(visible, scores, -jnp.inf)
            exponent = jnp.exp(scores - jnp.max(scores, axis=-1, keepdims=True))
            total = jnp.sum(exponent, axis=-1, keepdims=True)
            probs = (exponent / total).astype(BF16)
            head_own[:, span] = jnp.dot(
                probs, value_ref[...], preferred_element_type=F32
            ).astype(BF16)

    attend()
    for load in small[3:]:
        load.wait()
    pl.semaphore_wait(barrier, len(partners))

    count = [0]
    pending = []
    clock = [0]
    slots = []
    lines = {}

    def copy_of(src, dst, send_index, recv_index, target):
        return pltpu.make_async_remote_copy(
            src_ref=src,
            dst_ref=dst,
            send_sem=send_sems.at[send_index],
            recv_sem=recv_sems.at[recv_index],
            device_id=target,
            device_id_type=MESH,
        )

    def take(n):
        k = count[0]
        count[0] = k + n
        return k

    class Tracked:
        def __init__(self, src, dst, recv_index, target):
            free = [i for i, old in enumerate(slots) if old.sent]
            if free:
                slot = free[0]
            elif len(slots) < send_slots:
                slot = len(slots)
                slots.append(None)
            else:
                slot = min(range(send_slots), key=lambda i: slots[i].started)
                slots[slot].wait_send()
            clock[0] += 1
            self.started, self.ended, self.sent = clock[0], None, False
            self.index = recv_index
            self.copy = copy_of(src, dst, slot, recv_index, target)
            self.copy.start()
            slots[slot] = self
            pending.append(self)

        def wait_recv(self):
            self.copy.wait_recv()
            clock[0] += 1
            self.ended = clock[0]

        def wait_send(self):
            if not self.sent:
                self.copy.wait_send()
                self.sent = True

    def send(src, dst, target):
        past = lines.setdefault(id(target), [])
        index, seen = None, set()
        answered = max([m.started for m in past if m.ended is not None], default=0)
        for old in reversed(past):
            if old.index in seen:
                continue
            seen.add(old.index)
            if old.ended is not None and old.ended < answered:
                index = old.index
                break
        copy = Tracked(src, dst, take(1) if index is None else index, target)
        past.append(copy)
        return copy

    def send_planes(source, target):
        k = take(slabs)
        for p in others:
            Tracked(source(p), target(z), k + z, device(p, x, y, c))
        return lambda p: copy_of(target(p), target(p), 0, k + p, core)

    pieces = [(0, width // 2), (width // 2, width // 4), (3 * width // 4, width // 4)]
    proj_copy = []
    for start, size in pieces:
        cols = pl.ds(start, size)
        proj_copy.append(send(proj_ref.at[:, cols], proj_x.at[:, cols], over_x))
    above = device(jnp.minimum(z + 1, slabs - 1), x, y, c)
    below = device(jnp.maximum(z - 1, 0), x, y, c)
    is_low, is_high = z < slabs - 1, z > 0
    chunks = 4
    chunk = head_own.shape[1] // chunks
    chain = [take(slabs) for _ in range(chunks)]
    chain_sent = [send_slots + i * (slabs + 2) for i in range(chunks)]
    spans = [pl.ds(i * chunk, chunk) for i in range(chunks)]

    def own_copy(i, rising):
        return copy_of(
            head_own.at[:, spans[i]],
            heads.at[z, :, spans[i]],
            chain_sent[i] + slabs + (0 if rising else 1),
            chain[i] + z,
            above if rising else below,
        )

    def relay_copy(i, p, target):
        spot = heads.at[p, :, spans[i]]
        return copy_of(spot, spot, chain_sent[i] + p, chain[i] + p, target)

    def chain_do(i, p, act_on):
        if p is None:
            rising, falling = is_low, is_high
        else:
            rising, falling = (p < z) & is_low, (p > z) & is_high

        @pl.when(rising)
        def _():
            act_on(own_copy(i, True) if p is None else relay_copy(i, p, above))

        @pl.when(falling)
        def _():
            act_on(own_copy(i, False) if p is None else relay_copy(i, p, below))

    for i in range(chunks):
        chain_do(i, None, lambda copy: copy.start())

    def relay(p):
        for i in range(chunks):
            relay_copy(i, p, above).wait_recv()
            chain_do(i, p, lambda copy: copy.start())

    def project(k, weights, columns):
        source = head_own[...] if k == 0 else heads[planes[k]]
        got = jnp.dot(source, weights, preferred_element_type=F32)
        for yy in range(2):
            for cc in range(2):
                start = (yy * 2 + cc) * tok
                part[k, cc, yy, :, columns] = got[start : start + tok]

    def columns_of(i):
        if i == 0:
            return pl.ds(pl.multiple_of(x * width, width), width)
        start, size = pieces[i - 1]
        return pl.ds(pl.multiple_of((1 - x) * width + start, LANES), size)

    half_copy, y_copy = {}, {}

    def to_core(i, ks):
        columns = columns_of(i)
        half_copy[i, ks] = send(
            part.at[pl.ds(ks[0], len(ks)), 1 - c, :, :, columns],
            got_half.at[pl.ds(ks[0], len(ks)), :, :, columns],
            core,
        )

    def over_cores(i, ks):
        columns = columns_of(i)
        half_copy[i, ks].wait_recv()
        for k in ks:
            total = part[k, c, 1 - y, :, columns] + got_half[k, 1 - y, :, columns]
            sum_half[k, :, columns] = total.astype(BF16)
        spot = pl.ds(ks[0], len(ks))
        y_copy[i, ks] = send(
            sum_half.at[spot, :, columns], got_y.at[spot, :, columns], over_y
        )
        for k in ks:
            part[k, c, y, :, columns] = part[k, c, y, :, columns] + got_half[k, y, :, columns]

    half_tok = tok // 2

    def finish(i, ks):
        columns = columns_of(i)
        y_copy[i, ks].wait_recv()
        for k in ks:
            total = part[k, c, y, :, columns] + got_y[k, :, columns].astype(F32)
            total = (total + res_in[planes[k], :, columns].astype(F32)).astype(BF16)
            spot = pl.ds(pl.multiple_of(planes[k] * half_tok, half_tok), half_tok)
            for h in range(2):
                rows[z, x, y, c, h, spot, columns] = total[h * half_tok : (h + 1) * half_tok]

    def fold(k):
        loads[k].wait()

        @pl.loop(0, plane // LANES)
        def _(r):
            start = pl.multiple_of(planes[k] * plane + r * LANES, LANES)
            scale = jnp.broadcast_to(gain_ref[:, pl.ds(start, LANES)], (LANES, LANES)).T
            spot = pl.ds(pl.multiple_of(r * LANES, LANES), LANES)
            for n in range(ff2 // LANES):
                columns = slice(n * LANES, (n + 1) * LANES)
                value = gate_up[k, spot, columns].astype(F32) * scale
                gate_up[k, spot, columns] = value.astype(BF16)

    every = tuple(range(slabs))
    near = every[:-1]
    last = every[-1:]
    is_end = (z == 0) | (z == slabs - 1)

    def piece_of(i, ks):
        start, size = pieces[i - 1]
        for k in ks:
            project(k, proj_x[:, start : start + size], columns_of(i))
        to_core(i, ks)

    def own_piece(ks):
        for k in ks:
            project(k, proj_ref[...], columns_of(0))
        to_core(0, ks)

    fold(0)
    fold(1)
    res_in[z] = res_ref[:, plane_cols(z)]
    relay(planes[1])
    relay(planes[2])
    own_piece(near)
    fold(2)
    fold(3)

    @pl.when(jnp.logical_not(is_end))
    def _():
        relay(planes[3])

    proj_copy[0].wait_recv()
    piece_of(1, near)
    over_cores(0, near)
    over_cores(1, near)
    res_wait = send_planes(lambda p: res_ref.at[:, plane_cols(p)], lambda p: res_in.at[p])
    gate_wait = send_planes(lambda p: gates.at[z, x, y, c], lambda p: gates.at[p, x, y, c])

    @pl.when(is_end)
    def _():
        for i in range(chunks):
            relay_copy(i, planes[3], above).wait_recv()

    own_piece(last)
    piece_of(1, last)
    proj_copy[1].wait_recv()
    piece_of(2, every)
    over_cores(0, last)
    over_cores(1, last)
    over_cores(2, every)
    proj_copy[2].wait_recv()
    piece_of(3, every)
    for p in others:
        res_wait(p).wait_recv()
    finish(0, near)
    finish(1, near)
    finish(0, last)
    finish(1, last)
    over_cores(3, every)
    finish(2, every)
    finish(3, every)

    low, high = pl.ds(0, width), pl.ds(width, width)
    g_copy = {}

    def pass_on(kind, unit, spot, target):
        g_copy[kind, unit] = send(spot, spot, target)

    z_wait = {}

    def send_half(h):
        before = len(pending)
        z_wait[h] = send_planes(
            lambda p: rows.at[z, x, y, c, h], lambda p: rows.at[p, x, y, c, h]
        )
        for i, copy in enumerate(pending[before:]):
            g_copy["z", (h, i)] = copy

    for p in others:
        gate_wait(p).wait_recv()
    gate_x = send(gates.at[:, x, y, c], gates.at[:, x, y, c], over_x)
    gate_copy = {}

    def gates_y():
        gate_x.wait_recv()
        gate_copy["y"] = send(gates.at[:, :, y, c], gates.at[:, :, y, c], over_y)

    def gates_c():
        gate_copy["y"].wait_recv()
        gate_copy["c"] = send(gates.at[:, :, :, c], gates.at[:, :, :, c], core)

    def gates_done():
        gate_copy["c"].wait_recv()

    def first(h, k):
        p = planes[k]
        if k:
            z_wait[h](p).wait_recv()
        pass_on("x", (h, k), rows.at[p, x, y, c, h, :, low], over_x)
        pass_on("y", (h, k), rows.at[p, x, y, c, h, :, high], over_y)
        pass_on("c", (h, k), rows.at[p, x, y, c, h], core)

    def second_x(h, k):
        p = planes[k]
        g_copy["x", (h, k)].wait_recv()
        pass_on("xy", (h, k), rows.at[p, :, y, c, h, :, low], over_y)
        pass_on("xc", (h, k), rows.at[p, 1 - x, y, c, h, :, low], core)

    def second_y(h, k):
        p = planes[k]
        g_copy["y", (h, k)].wait_recv()
        pass_on("yx", (h, k), rows.at[p, x, :, c, h, :, high], over_x)
        pass_on("yc", (h, k), rows.at[p, x, 1 - y, c, h, :, high], core)

    def third_x(h, k):
        p = planes[k]
        g_copy["xy", (h, k)].wait_recv()
        pass_on("xyc", (h, k), rows.at[p, :, 1 - y, c, h, :, low], core)

    def third_y(h, k):
        p = planes[k]
        g_copy["yx", (h, k)].wait_recv()
        pass_on("yxc", (h, k), rows.at[p, 1 - x, :, c, h, :, high], core)

    step = 512
    half_rows = 8 * slabs * half_tok

    def up_project(h, k):
        for kind in ("c", "xc", "yc", "xyc", "yxc"):
            g_copy[kind, (h, k)].wait_recv()
        p = planes[k]
        per = block // 2 // tok

        @pl.loop(0, 8)
        def _(b):
            for s in range(per):
                spot = pl.ds(s * tok, tok)
                value = rows[p, b // 4, (b // 2) % 2, b % 2, h, spot, :].astype(F32)
                place = pl.ds(pl.multiple_of((b * per + s) * tok, tok), tok)
                square = squares[h, place, :]
                for i in range(plane // LANES):
                    strip = value[:, i * LANES : (i + 1) * LANES]
                    square = square + strip * strip
                squares[h, place, :] = square

        @pl.loop(0, ff2 // step)
        def _(n):
            columns = pl.ds(pl.multiple_of(n * step, step), step)
            tokens = rows[p, :, :, :, h].reshape(half_rows, plane)
            got = jnp.dot(tokens, gate_up[k, :, columns], preferred_element_type=F32)
            if k:
                acc[h, :, columns] = acc[h, :, columns] + got
            else:
                acc[h, :, columns] = got

    me = g * 4 + t
    half_lane = lax.broadcasted_iota(jnp.int32, (half_tok, LANES), 1)
    picked = (half_lane == me) | (half_lane == me + experts)

    def clear(h):
        own = pl.ds(pl.multiple_of(z * half_tok, half_tok), half_tok)
        for q in range(slabs):
            hidden[q, h * half_tok : (h + 1) * half_tok] = rows[q, x, y, c, h, own, :]
        for (kind, unit), copy in g_copy.items():
            if unit[0] == h:
                copy.wait_send()

    def spots(k):
        return pl.ds(k * half_tok, half_tok)

    cut = 3 * plane // 8 // LANES * LANES
    part_a, part_d = pl.ds(0, cut), pl.ds(cut, plane - cut)
    c_copy, x_copy, y2_copy, d_copy, a_copy = {}, {}, {}, {}, {}
    zk = {h: take(2 * slabs) for h in range(2)}
    chunk_rows = slabs * half_tok

    def down_act(h):
        for cc in range(2):
            for k in range(slabs):
                p = planes[k]
                for xx in range(2):
                    for yy in range(2):
                        source = c if cc == 0 else 1 - c
                        b = xx * 4 + yy * 2 + source
                        place = pl.ds(
                            pl.multiple_of((b * slabs + p) * half_tok, half_tok), half_tok
                        )
                        mean = jnp.sum(squares[h, place, :], axis=-1, keepdims=True)
                        scale = lax.rsqrt(mean * (1.0 / model) + 1e-06)
                        mine = gates[p, xx, yy, source, h * half_tok : (h + 1) * half_tok]
                        share = jnp.sum(
                            jnp.where(picked, mine.astype(F32), 0.0), axis=-1, keepdims=True
                        )
                        left = acc[h, place, :ff] * scale
                        right = acc[h, place, ff:] * (scale * share)
                        value = left / (1.0 + jnp.exp(-left)) * right
                        spot = ((cc * 2 + xx) * 2 + yy) * chunk_rows + k * half_tok
                        act[spot : spot + half_tok, :] = value.astype(BF16)
        if h == 0:
            loads[slabs].wait()

    def down_project(h, q):
        tile = plane // 2

        @pl.loop(2 * q, 2 * q + 2)
        def _(n):
            got = jnp.dot(
                act[...],
                down[:, pl.ds(pl.multiple_of(n * tile, tile), tile)],
                preferred_element_type=F32,
            ).astype(BF16)
            columns = pl.ds(pl.multiple_of((n % 2) * tile, tile), tile)
            for cc in range(2):
                for xx in range(2):
                    for yy in range(2):
                        spot = ((cc * 2 + xx) * 2 + yy) * chunk_rows
                        rows[q, xx, yy, 1 - cc, h, :, columns] = got[spot : spot + chunk_rows]

        c_copy[h, q] = send(rows.at[q, :, :, 0, h], got_core.at[q, :, :, h], core)

    def add_into(ref, other):
        count_rows = ref.shape[0]
        for start in range(0, count_rows, 32):
            spot = slice(start, start + 32)
            ref[spot, :] = (ref[spot, :].astype(F32) + other[spot, :].astype(F32)).astype(BF16)

    def add_cores(h, q):
        c_copy[h, q].wait_recv()
        for xx in range(2):
            for yy in range(2):
                add_into(rows.at[q, xx, yy, 1, h], got_core.at[q, xx, yy, h])
        x_copy[h, q] = send(rows.at[q, 1 - x, :, 1, h, :, part_d], got_x.at[q, :, h], over_x)
        y2_copy[h, q] = send(rows.at[q, :, 1 - y, 1, h, :, part_a], got_y2.at[q, :, h], over_y)

    def send_home(h, q, source, landing, index):
        for k in range(1, slabs):
            Tracked(source(k), landing.at[z, h, q], zk[h] + index + z, device(planes[k], x, y, c))

    def landed(h, landing, index):
        for p in others:
            spot = landing.at[p, h]
            copy_of(spot, spot, 0, zk[h] + index + p, core).wait_recv()

    def add_a(h, q):
        y2_copy[h, q].wait_recv()
        for xx in range(2):
            add_into(rows.at[q, xx, y, 1, h, :, part_a], got_y2.at[q, xx, h])
        send_home(h, q, lambda k: rows.at[q, :, y, 1, h, spots(k), part_a], landed_a, 0)

    def add_d(h, q):
        x_copy[h, q].wait_recv()
        for yy in range(2):
            add_into(rows.at[q, x, yy, 1, h, :, part_d], got_x.at[q, yy, h])
        d_copy[h, q] = send(rows.at[q, x, 1 - y, 1, h, :, part_d], last_d.at[q, h], over_y)

    def add_last(h, q):
        d_copy[h, q].wait_recv()
        add_into(rows.at[q, x, y, 1, h, :, part_d], last_d.at[q, h])
        send_home(h, q, lambda k: rows.at[q, x, y, 1, h, spots(k), part_d], landed_d, slabs)

    def landed_sum(h):
        landed(h, landed_a, 0)
        for q in range(slabs):
            for xx in range(2):
                total = rows[q, xx, y, 1, h, spots(0), part_a].astype(F32)
                for p in others:
                    total = total + landed_a[p, h, q, xx].astype(F32)
                rows[q, xx, y, 1, h, spots(0), part_a] = total.astype(BF16)
        a_copy[h] = send(
            rows.at[:, 1 - x, y, 1, h, spots(0), part_a], last_a.at[h], over_x
        )

    def output(h):
        place = slice(h * half_tok, (h + 1) * half_tok)
        a_copy[h].wait_recv()
        for q in range(slabs):
            total = hidden[q, place, part_a].astype(F32)
            total = total + rows[q, x, y, 1, h, spots(0), part_a].astype(F32)
            total = total + last_a[h, q].astype(F32)
            out_ref[place, q * plane : q * plane + cut] = total.astype(BF16)
        landed(h, landed_d, slabs)
        for q in range(slabs):
            total = hidden[q, place, part_d].astype(F32)
            total = total + rows[q, x, y, 1, h, spots(0), part_d].astype(F32)
            for p in others:
                total = total + landed_d[p, h, q].astype(F32)
            out_ref[place, q * plane + cut : (q + 1) * plane] = total.astype(BF16)

    send_half(0)
    first(0, 0)
    first(1, 0)
    second_y(0, 0)
    second_x(0, 0)
    second_x(1, 0)
    second_y(1, 0)
    first(0, 1)
    send_half(1)
    third_y(0, 0)
    third_x(0, 0)
    gates_y()
    up_project(0, 0)
    first(0, 2)
    third_y(1, 0)
    third_x(1, 0)
    second_x(0, 1)
    second_y(0, 1)
    first(0, 3)
    gates_c()
    up_project(1, 0)
    second_y(0, 2)
    second_x(0, 2)
    first(1, 1)
    third_y(0, 1)
    third_x(0, 1)
    second_y(0, 3)
    second_x(0, 3)
    up_project(0, 1)
    first(1, 2)
    third_y(0, 2)
    third_x(0, 2)
    second_y(1, 1)
    second_x(1, 1)
    up_project(0, 2)
    first(1, 3)
    third_y(0, 3)
    third_x(0, 3)
    second_y(1, 2)
    second_x(1, 2)
    up_project(0, 3)
    gates_done()
    clear(0)
    down_act(0)
    third_x(1, 1)
    third_y(1, 1)
    down_project(0, 0)
    second_x(1, 3)
    second_y(1, 3)
    down_project(0, 1)
    down_project(0, 2)
    third_x(1, 2)
    third_y(1, 2)
    add_cores(0, 0)
    down_project(0, 3)
    add_cores(0, 1)
    up_project(1, 1)
    third_y(1, 3)
    third_x(1, 3)
    add_cores(0, 2)
    add_cores(0, 3)
    up_project(1, 2)
    add_a(0, 0)
    add_d(0, 0)
    add_a(0, 1)
    up_project(1, 3)
    add_a(0, 2)
    clear(1)
    down_act(1)
    add_d(0, 1)
    down_project(1, 0)
    add_a(0, 3)
    down_project(1, 1)
    add_last(0, 0)
    down_project(1, 2)
    add_d(0, 2)
    add_cores(1, 0)
    add_last(0, 1)
    down_project(1, 3)
    add_cores(1, 1)
    add_cores(1, 2)
    add_d(0, 3)
    landed_sum(0)
    add_cores(1, 3)
    add_last(0, 2)
    add_a(1, 0)
    add_d(1, 0)
    add_a(1, 1)
    add_a(1, 2)
    add_d(1, 1)
    add_last(0, 3)
    add_d(1, 2)
    add_a(1, 3)
    add_last(1, 0)
    add_last(1, 1)
    add_d(1, 3)
    landed_sum(1)
    add_last(1, 2)
    add_last(1, 3)
    output(0)
    output(1)
    for copy in pending:
        copy.wait_send()
    for i in range(chunks):
        chain_do(i, None, lambda copy: copy.wait_send())
        for p in others:
            chain_do(i, p, lambda copy: copy.wait_send())
    assert count[0] <= copies_max, count[0]


def layer(queries, keys, values, docs, out_proj, residual, gain, ids, weights, gate_up, down, groups):
    slabs = groups // 2
    tok, model = residual.shape
    tokens, depth = queries.shape
    plane = model // slabs
    ff, ff2 = down.shape[0], gate_up.shape[1]
    total = tok * slabs * 8
    half = slabs * tok // 2
    cut = 3 * plane // 8 // LANES * LANES
    copies_max = 88
    send_slots = 48
    dma = pltpu.SemaphoreType.DMA
    vmem = pl.BlockSpec(memory_space=pltpu.VMEM)
    hbm = pl.BlockSpec(memory_space=pl.ANY)
    return pl.pallas_call(
        functools.partial(layer_kernel, slabs, copies_max, send_slots),
        out_shape=jax.ShapeDtypeStruct((tok, model), BF16),
        in_specs=[hbm] * 3 + [vmem] + [hbm] * 2 + [vmem] * 3 + [hbm] * 2,
        out_specs=vmem,
        scratch_shapes=[
            pltpu.VMEM(queries.shape, BF16),
            pltpu.VMEM(keys.shape, BF16),
            pltpu.VMEM(values.shape, BF16),
            pltpu.VMEM(out_proj.shape, BF16),
            pltpu.VMEM(residual.shape, BF16),
            pltpu.VMEM((tokens, depth), BF16),
            pltpu.VMEM(out_proj.shape, BF16),
            pltpu.VMEM((slabs, tokens, depth), BF16),
            pltpu.VMEM((slabs, tok, plane), BF16),
            pltpu.VMEM((slabs, 2, 2, tok, plane), F32),
            pltpu.VMEM((slabs, 2, tok, plane), F32),
            pltpu.VMEM((slabs, tok, plane), BF16),
            pltpu.VMEM((slabs, tok, plane), BF16),
            pltpu.VMEM((ids.shape[0], LANES), jnp.int32),
            pltpu.VMEM((ids.shape[0], LANES), F32),
            pltpu.VMEM((slabs, 2, 2, 2, tok, LANES), BF16),
            pltpu.VMEM((slabs, 2, 2, 2, 2, half, plane), BF16),
            pltpu.VMEM((2, total // 2, LANES), F32),
            pltpu.VMEM((2, total // 2, ff2), F32),
            pltpu.VMEM((total // 2, ff), BF16),
            pltpu.VMEM((slabs, plane, ff2), BF16),
            pltpu.VMEM((ff, model), BF16),
            pltpu.VMEM((slabs, tok, plane), BF16),
            pltpu.VMEM((slabs, 2, 2, 2, half, plane), BF16),
            pltpu.VMEM((slabs, 2, 2, half, plane - cut), BF16),
            pltpu.VMEM((slabs, 2, 2, half, cut), BF16),
            pltpu.VMEM((slabs, 2, half, plane - cut), BF16),
            pltpu.VMEM((2, slabs, tok // 2, cut), BF16),
            pltpu.VMEM((slabs, 2, slabs, 2, tok // 2, cut), BF16),
            pltpu.VMEM((slabs, 2, slabs, tok // 2, plane - cut), BF16),
            dma((slabs + 6,)),
            dma((send_slots + 4 * (slabs + 2),)),
            dma((copies_max,)),
        ],
        compiler_params=pltpu.CompilerParams(
            collective_id=0, has_side_effects=True, vmem_limit_bytes=VMEM_LIMIT
        ),
    )(queries, keys, values, docs, out_proj, residual, gain, ids, weights, gate_up, down)


def spread_gates(expert_ids, gate_weights, experts):
    gates = jnp.sum(
        jnp.where(
            expert_ids[:, :, None] == jnp.arange(experts, dtype=jnp.int32)[None, None, :],
            gate_weights[:, :, None],
            0.0,
        ),
        axis=1,
    )
    high = lax.reduce_precision(gates, 8, 7)
    low = gates - high
    pad = -(2 * experts) % LANES
    return jnp.concatenate(
        [high, low, jnp.zeros((gates.shape[0], pad), F32)], axis=1
    ).astype(BF16)


def plain_layer(head_out, out_proj, residual, gain, extra, gate_up, down, groups, tensors):
    experts = groups * tensors
    tok, model = residual.shape
    heads = lax.all_gather(head_out, "group", axis=0, tiled=True)
    part = jnp.dot(heads, out_proj, preferred_element_type=F32)
    part = part.reshape(groups, tensors, tok, part.shape[1])
    part = lax.psum_scatter(part, "tensor", scatter_dimension=1, tiled=False)
    attended = lax.all_to_all(part, "group", split_axis=0, concat_axis=2, tiled=True)
    hidden = residual.astype(F32) + attended.reshape(tok, model)
    mean_square = jnp.mean(hidden * hidden, axis=-1, keepdims=True)
    normed = (hidden * lax.rsqrt(mean_square + 1e-06) * gain).astype(BF16)
    rows = jnp.concatenate([normed, extra], axis=1)
    rows_all = lax.all_gather(rows, ("group", "tensor"), axis=0, tiled=True)
    me = lax.axis_index("group") * tensors + lax.axis_index("tensor")
    lane = jnp.arange(extra.shape[1], dtype=jnp.int32)
    picked = (lane == me) | (lane == me + experts)
    gate_col = jnp.sum(
        jnp.where(picked[None, :], rows_all[:, model:].astype(F32), 0.0), axis=1, keepdims=True
    )
    ff = down.shape[0]
    projected = jnp.dot(rows_all[:, :model], gate_up, preferred_element_type=F32)
    activated = (jax.nn.silu(projected[:, :ff]) * projected[:, ff:]).astype(BF16)
    expert_out = jnp.dot(activated, down, preferred_element_type=F32)
    weighted = (expert_out * gate_col).astype(BF16)
    expert_sum = lax.psum_scatter(weighted, ("group", "tensor"), scatter_dimension=0, tiled=True)
    return (hidden + expert_sum.astype(F32)).astype(BF16)


def on_device(
    queries,
    keys,
    values,
    document_index,
    out_proj,
    residual_in,
    norm_gain,
    expert_ids,
    gate_weights,
    w_gate_up,
    w_down,
):
    groups, tensors = lax.axis_size("group"), lax.axis_size("tensor")
    gain = norm_gain[None, :]
    if groups == 8 and tensors == 4:
        return layer(
            queries,
            keys,
            values,
            document_index,
            out_proj,
            residual_in,
            gain,
            expert_ids.T,
            gate_weights.T,
            w_gate_up[0],
            w_down[0],
            groups,
        )
    head_out = attention(queries, keys, values, document_index)
    extra = spread_gates(expert_ids, gate_weights, groups * tensors)
    return plain_layer(
        head_out, out_proj, residual_in, gain, extra, w_gate_up[0], w_down[0], groups, tensors
    )


def solution(mesh):
    in_specs = (
        P("group", "tensor"),
        P("group", "tensor"),
        P("group", "tensor"),
        P("group", None),
        P("tensor", "group"),
        P(("group", "tensor"), None),
        P(),
        P(("group", "tensor"), None),
        P(("group", "tensor"), None),
        P(("group", "tensor"), None, None),
        P(("group", "tensor"), None, None),
    )
    out_specs = P(("group", "tensor"), None)
    return jax.shard_map(
        on_device, mesh=mesh, in_specs=in_specs, out_specs=out_specs, check_vma=False
    )
```

```python
import functools

import jax
import jax.numpy as jnp
from jax import lax
from jax.experimental import pallas as pl
from jax.experimental.pallas import tpu as pltpu
from jax.sharding import PartitionSpec as P

HEAD_SIZE = 128
LANES = 128
MESH = pl.DeviceIdType.MESH
VMEM_LIMIT = 62 * 1024 * 1024
F32 = jnp.float32
BF16 = jnp.bfloat16


def attention(queries, keys, values, document_index):
    token_group = queries.shape[0]
    kv_dev = keys.shape[1] // HEAD_SIZE
    query_dev = queries.shape[1] // HEAD_SIZE
    group_ratio = query_dev // kv_dev
    query_head_split = queries.reshape(token_group, kv_dev, group_ratio, HEAD_SIZE)
    key_head_split = keys.reshape(token_group, kv_dev, HEAD_SIZE)
    value_head_split = values.reshape(token_group, kv_dev, HEAD_SIZE)
    scores = jnp.einsum(
        "qgrd,kgd->grqk", query_head_split, key_head_split, preferred_element_type=F32
    ) * (1.0 / HEAD_SIZE**0.5)
    doc_row = document_index[0]
    positions = jnp.arange(token_group, dtype=jnp.int32)
    visible = (positions[:, None] >= positions[None, :]) & (doc_row[:, None] == doc_row[None, :])
    scores = jnp.where(visible, scores, -jnp.inf)
    row_max = jnp.max(scores, axis=-1, keepdims=True)
    exponent = jnp.where(visible, jnp.exp(scores - row_max), 0.0)
    weights = (exponent / jnp.sum(exponent, axis=-1, keepdims=True)).astype(BF16)
    head_out = jnp.einsum("grqk,kgd->qgrd", weights, value_head_split, preferred_element_type=F32)
    return head_out.astype(BF16).reshape(token_group, query_dev * HEAD_SIZE)


def device(z, x, y, c):
    return (z * 2 + x, y * 2 + c)


def nearest_first(z):
    first = jnp.where(z == 0, 1, jnp.where(z == 1, 2, jnp.where(z == 2, 1, 2)))
    second = jnp.where(z == 0, 2, jnp.where(z == 1, 0, jnp.where(z == 2, 3, 1)))
    third = jnp.where(z <= 1, 3, 0)
    return [first, second, third]


def layer_kernel(
    slabs,
    copies_max,
    send_slots,
    query_hbm,
    key_hbm,
    value_hbm,
    doc_ref,
    proj_hbm,
    res_hbm,
    gain_ref,
    ids_ref,
    weight_ref,
    gate_up_hbm,
    down_hbm,
    out_ref,
    query_ref,
    key_ref,
    value_ref,
    proj_ref,
    res_ref,
    head_own,
    proj_x,
    heads,
    res_in,
    part,
    got_half,
    sum_half,
    got_y,
    ids_pad,
    weight_pad,
    gates,
    rows,
    squares,
    acc,
    act,
    gate_up,
    down,
    hidden,
    got_core,
    got_x,
    got_y2,
    last_d,
    last_a,
    landed_a,
    landed_d,
    load_sem,
    send_sems,
    recv_sems,
):
    g, t = lax.axis_index("group"), lax.axis_index("tensor")
    z, x, y, c = g // 2, g % 2, t // 2, t % 2
    tok, model = res_ref.shape
    plane = model // slabs
    width = plane // 2
    ff2 = gate_up.shape[2]
    ff = ff2 // 2
    experts = slabs * 8
    block = slabs * tok
    others = nearest_first(z)
    planes = [z] + others
    core, over_y, over_x = device(z, x, y, 1 - c), device(z, x, 1 - y, c), device(z, 1 - x, y, c)

    def plane_cols(p):
        return pl.ds(pl.multiple_of(p * plane, plane), plane)

    small = [
        pltpu.make_async_copy(source, target, load_sem.at[slabs + 1 + i])
        for i, (source, target) in enumerate(
            [
                (key_hbm, key_ref),
                (query_hbm, query_ref),
                (value_hbm, value_ref),
                (proj_hbm, proj_ref),
                (res_hbm, res_ref),
            ]
        )
    ]
    for load in small:
        load.start()
    barrier = pltpu.get_barrier_semaphore()
    partners = [core, over_y, over_x] + [device(p, x, y, c) for p in others]
    for partner in partners:
        pl.semaphore_signal(barrier, inc=1, device_id=partner, device_id_type=MESH)
    loads = [
        pltpu.make_async_copy(
            gate_up_hbm.at[pl.ds(pl.multiple_of(planes[k] * plane, plane), plane)],
            gate_up.at[k],
            load_sem.at[k],
        )
        for k in range(slabs)
    ]
    loads.append(pltpu.make_async_copy(down_hbm, down, load_sem.at[slabs]))

    ids_pad[...] = jnp.zeros_like(ids_pad)
    weight_pad[...] = jnp.zeros_like(weight_pad)
    ids_pad[:, :tok] = ids_ref[...]
    weight_pad[:, :tok] = weight_ref[...]
    expert = lax.broadcasted_iota(jnp.int32, (LANES, LANES), 0)
    gate = jnp.zeros((LANES, LANES), F32)
    for k in range(ids_ref.shape[0]):
        chosen = ids_pad[k : k + 1, :]
        hit = (expert == chosen) | (expert == chosen + experts)
        gate = gate + jnp.where(hit, weight_pad[k : k + 1, :], 0.0)
    gate_high = gate.astype(BF16).astype(F32)
    gate = jnp.where(expert < experts, gate_high, gate - gate_high)
    gates[z, x, y, c] = gate.T[:tok].astype(BF16)
    squares[...] = jnp.zeros_like(squares)

    for load in small[:3]:
        load.wait()
    for load in loads:
        load.start()

    def attend():
        tokens = query_ref.shape[0]
        doc = jnp.broadcast_to(doc_ref[...].astype(F32), (tokens, tokens))
        row = lax.broadcasted_iota(jnp.int32, (tokens, tokens), 0)
        column = lax.broadcasted_iota(jnp.int32, (tokens, tokens), 1)
        visible = (row >= column) & (doc == doc.T)
        for h in range(query_ref.shape[1] // HEAD_SIZE):
            span = slice(h * HEAD_SIZE, (h + 1) * HEAD_SIZE)
            scores = lax.dot_general(
                query_ref[:, span],
                key_ref[...],
                (((1,), (1,)), ((), ())),
                preferred_element_type=F32,
            ) * (1.0 / HEAD_SIZE**0.5)
            scores = jnp.where(visible, scores, -jnp.inf)
            exponent = jnp.exp(scores - jnp.max(scores, axis=-1, keepdims=True))
            total = jnp.sum(exponent, axis=-1, keepdims=True)
            probs = (exponent / total).astype(BF16)
            head_own[:, span] = jnp.dot(
                probs, value_ref[...], preferred_element_type=F32
            ).astype(BF16)

    attend()
    for load in small[3:]:
        load.wait()
    pl.semaphore_wait(barrier, len(partners))

    count = [0]
    pending = []
    clock = [0]
    slots = []
    lines = {}

    def copy_of(src, dst, send_index, recv_index, target):
        return pltpu.make_async_remote_copy(
            src_ref=src,
            dst_ref=dst,
            send_sem=send_sems.at[send_index],
            recv_sem=recv_sems.at[recv_index],
            device_id=target,
            device_id_type=MESH,
        )

    def take(n):
        k = count[0]
        count[0] = k + n
        return k

    class Tracked:
        def __init__(self, src, dst, recv_index, target):
            free = [i for i, old in enumerate(slots) if old.sent]
            if free:
                slot = free[0]
            elif len(slots) < send_slots:
                slot = len(slots)
                slots.append(None)
            else:
                slot = min(range(send_slots), key=lambda i: slots[i].started)
                slots[slot].wait_send()
            clock[0] += 1
            self.started, self.ended, self.sent = clock[0], None, False
            self.index = recv_index
            self.copy = copy_of(src, dst, slot, recv_index, target)
            self.copy.start()
            slots[slot] = self
            pending.append(self)

        def wait_recv(self):
            self.copy.wait_recv()
            clock[0] += 1
            self.ended = clock[0]

        def wait_send(self):
            if not self.sent:
                self.copy.wait_send()
                self.sent = True

    def send(src, dst, target):
        past = lines.setdefault(id(target), [])
        index, seen = None, set()
        answered = max([m.started for m in past if m.ended is not None], default=0)
        for old in reversed(past):
            if old.index in seen:
                continue
            seen.add(old.index)
            if old.ended is not None and old.ended < answered:
                index = old.index
                break
        copy = Tracked(src, dst, take(1) if index is None else index, target)
        past.append(copy)
        return copy

    def send_planes(source, target):
        k = take(slabs)
        for p in others:
            Tracked(source(p), target(z), k + z, device(p, x, y, c))
        return lambda p: copy_of(target(p), target(p), 0, k + p, core)

    pieces = [(0, width // 2), (width // 2, width // 4), (3 * width // 4, width // 4)]
    proj_copy = []
    for start, size in pieces:
        cols = pl.ds(start, size)
        proj_copy.append(send(proj_ref.at[:, cols], proj_x.at[:, cols], over_x))
    above = device(jnp.minimum(z + 1, slabs - 1), x, y, c)
    below = device(jnp.maximum(z - 1, 0), x, y, c)
    is_low, is_high = z < slabs - 1, z > 0
    chunks = 4
    chunk = head_own.shape[1] // chunks
    chain = [take(slabs) for _ in range(chunks)]
    chain_sent = [send_slots + i * (slabs + 2) for i in range(chunks)]
    spans = [pl.ds(i * chunk, chunk) for i in range(chunks)]

    def own_copy(i, rising):
        return copy_of(
            head_own.at[:, spans[i]],
            heads.at[z, :, spans[i]],
            chain_sent[i] + slabs + (0 if rising else 1),
            chain[i] + z,
            above if rising else below,
        )

    def relay_copy(i, p, target):
        spot = heads.at[p, :, spans[i]]
        return copy_of(spot, spot, chain_sent[i] + p, chain[i] + p, target)

    def chain_do(i, p, act_on):
        if p is None:
            rising, falling = is_low, is_high
        else:
            rising, falling = (p < z) & is_low, (p > z) & is_high

        @pl.when(rising)
        def _():
            act_on(own_copy(i, True) if p is None else relay_copy(i, p, above))

        @pl.when(falling)
        def _():
            act_on(own_copy(i, False) if p is None else relay_copy(i, p, below))

    for i in range(chunks):
        chain_do(i, None, lambda copy: copy.start())

    def relay(p):
        for i in range(chunks):
            relay_copy(i, p, above).wait_recv()
            chain_do(i, p, lambda copy: copy.start())

    def project(k, weights, columns):
        source = head_own[...] if k == 0 else heads[planes[k]]
        got = jnp.dot(source, weights, preferred_element_type=F32)
        for yy in range(2):
            for cc in range(2):
                start = (yy * 2 + cc) * tok
                part[k, cc, yy, :, columns] = got[start : start + tok]

    def columns_of(i):
        if i == 0:
            return pl.ds(pl.multiple_of(x * width, width), width)
        start, size = pieces[i - 1]
        return pl.ds(pl.multiple_of((1 - x) * width + start, LANES), size)

    half_copy, y_copy = {}, {}

    def to_core(i, ks):
        columns = columns_of(i)
        half_copy[i, ks] = send(
            part.at[pl.ds(ks[0], len(ks)), 1 - c, :, :, columns],
            got_half.at[pl.ds(ks[0], len(ks)), :, :, columns],
            core,
        )

    def over_cores(i, ks):
        columns = columns_of(i)
        half_copy[i, ks].wait_recv()
        for k in ks:
            total = part[k, c, 1 - y, :, columns] + got_half[k, 1 - y, :, columns]
            sum_half[k, :, columns] = total.astype(BF16)
        spot = pl.ds(ks[0], len(ks))
        y_copy[i, ks] = send(
            sum_half.at[spot, :, columns], got_y.at[spot, :, columns], over_y
        )
        for k in ks:
            part[k, c, y, :, columns] = part[k, c, y, :, columns] + got_half[k, y, :, columns]

    half_tok = tok // 2

    def finish(i, ks):
        columns = columns_of(i)
        y_copy[i, ks].wait_recv()
        for k in ks:
            total = part[k, c, y, :, columns] + got_y[k, :, columns].astype(F32)
            total = (total + res_in[planes[k], :, columns].astype(F32)).astype(BF16)
            spot = pl.ds(pl.multiple_of(planes[k] * half_tok, half_tok), half_tok)
            for h in range(2):
                rows[z, x, y, c, h, spot, columns] = total[h * half_tok : (h + 1) * half_tok]

    def fold(k):
        loads[k].wait()

        @pl.loop(0, plane // LANES)
        def _(r):
            start = pl.multiple_of(planes[k] * plane + r * LANES, LANES)
            scale = jnp.broadcast_to(gain_ref[:, pl.ds(start, LANES)], (LANES, LANES)).T
            spot = pl.ds(pl.multiple_of(r * LANES, LANES), LANES)
            for n in range(ff2 // LANES):
                columns = slice(n * LANES, (n + 1) * LANES)
                value = gate_up[k, spot, columns].astype(F32) * scale
                gate_up[k, spot, columns] = value.astype(BF16)

    every = tuple(range(slabs))
    near = every[:-1]
    last = every[-1:]
    is_end = (z == 0) | (z == slabs - 1)

    def piece_of(i, ks):
        start, size = pieces[i - 1]
        for k in ks:
            project(k, proj_x[:, start : start + size], columns_of(i))
        to_core(i, ks)

    def own_piece(ks):
        for k in ks:
            project(k, proj_ref[...], columns_of(0))
        to_core(0, ks)

    fold(0)
    fold(1)
    res_in[z] = res_ref[:, plane_cols(z)]
    relay(planes[1])
    relay(planes[2])
    own_piece(near)
    fold(2)
    fold(3)

    @pl.when(jnp.logical_not(is_end))
    def _():
        relay(planes[3])

    proj_copy[0].wait_recv()
    piece_of(1, near)
    over_cores(0, near)
    over_cores(1, near)
    res_wait = send_planes(lambda p: res_ref.at[:, plane_cols(p)], lambda p: res_in.at[p])
    gate_wait = send_planes(lambda p: gates.at[z, x, y, c], lambda p: gates.at[p, x, y, c])

    @pl.when(is_end)
    def _():
        for i in range(chunks):
            relay_copy(i, planes[3], above).wait_recv()

    own_piece(last)
    piece_of(1, last)
    proj_copy[1].wait_recv()
    piece_of(2, every)
    over_cores(0, last)
    over_cores(1, last)
    over_cores(2, every)
    proj_copy[2].wait_recv()
    piece_of(3, every)
    for p in others:
        res_wait(p).wait_recv()
    finish(0, near)
    over_cores(3, every)
    finish(1, near)
    finish(0, last)
    finish(1, last)
    finish(2, every)
    finish(3, every)

    low, high = pl.ds(0, width), pl.ds(width, width)
    g_copy = {}

    def pass_on(kind, unit, spot, target):
        g_copy[kind, unit] = send(spot, spot, target)

    z_wait = {}

    def send_half(h):
        before = len(pending)
        z_wait[h] = send_planes(
            lambda p: rows.at[z, x, y, c, h], lambda p: rows.at[p, x, y, c, h]
        )
        for i, copy in enumerate(pending[before:]):
            g_copy["z", (h, i)] = copy

    for p in others:
        gate_wait(p).wait_recv()
    gate_x = send(gates.at[:, x, y, c], gates.at[:, x, y, c], over_x)
    gate_copy = {}

    def gates_y():
        gate_x.wait_recv()
        gate_copy["y"] = send(gates.at[:, :, y, c], gates.at[:, :, y, c], over_y)

    def gates_c():
        gate_copy["y"].wait_recv()
        gate_copy["c"] = send(gates.at[:, :, :, c], gates.at[:, :, :, c], core)

    def gates_done():
        gate_copy["c"].wait_recv()

    def first(h, k):
        p = planes[k]
        if k:
            z_wait[h](p).wait_recv()
        pass_on("x", (h, k), rows.at[p, x, y, c, h, :, low], over_x)
        pass_on("y", (h, k), rows.at[p, x, y, c, h, :, high], over_y)
        pass_on("c", (h, k), rows.at[p, x, y, c, h], core)

    def second_x(h, k):
        p = planes[k]
        g_copy["x", (h, k)].wait_recv()
        pass_on("xy", (h, k), rows.at[p, :, y, c, h, :, low], over_y)
        pass_on("xc", (h, k), rows.at[p, 1 - x, y, c, h, :, low], core)

    def second_y(h, k):
        p = planes[k]
        g_copy["y", (h, k)].wait_recv()
        pass_on("yx", (h, k), rows.at[p, x, :, c, h, :, high], over_x)
        pass_on("yc", (h, k), rows.at[p, x, 1 - y, c, h, :, high], core)

    def third_x(h, k):
        p = planes[k]
        g_copy["xy", (h, k)].wait_recv()
        pass_on("xyc", (h, k), rows.at[p, :, 1 - y, c, h, :, low], core)

    def third_y(h, k):
        p = planes[k]
        g_copy["yx", (h, k)].wait_recv()
        pass_on("yxc", (h, k), rows.at[p, 1 - x, :, c, h, :, high], core)

    step = 512
    half_rows = 8 * slabs * half_tok

    def up_project(h, k):
        for kind in ("c", "xc", "yc", "xyc", "yxc"):
            g_copy[kind, (h, k)].wait_recv()
        p = planes[k]
        per = block // 2 // tok

        @pl.loop(0, 8)
        def _(b):
            for s in range(per):
                spot = pl.ds(s * tok, tok)
                value = rows[p, b // 4, (b // 2) % 2, b % 2, h, spot, :].astype(F32)
                place = pl.ds(pl.multiple_of((b * per + s) * tok, tok), tok)
                square = squares[h, place, :]
                for i in range(plane // LANES):
                    strip = value[:, i * LANES : (i + 1) * LANES]
                    square = square + strip * strip
                squares[h, place, :] = square

        @pl.loop(0, ff2 // step)
        def _(n):
            columns = pl.ds(pl.multiple_of(n * step, step), step)
            tokens = rows[p, :, :, :, h].reshape(half_rows, plane)
            got = jnp.dot(tokens, gate_up[k, :, columns], preferred_element_type=F32)
            if k:
                acc[h, :, columns] = acc[h, :, columns] + got
            else:
                acc[h, :, columns] = got

    me = g * 4 + t
    half_lane = lax.broadcasted_iota(jnp.int32, (half_tok, LANES), 1)
    picked = (half_lane == me) | (half_lane == me + experts)

    def clear(h):
        own = pl.ds(pl.multiple_of(z * half_tok, half_tok), half_tok)
        for q in range(slabs):
            hidden[q, h * half_tok : (h + 1) * half_tok] = rows[q, x, y, c, h, own, :]
        for (kind, unit), copy in g_copy.items():
            if unit[0] == h:
                copy.wait_send()

    def spots(k):
        return pl.ds(k * half_tok, half_tok)

    cut = 3 * plane // 8 // LANES * LANES
    part_a, part_d = pl.ds(0, cut), pl.ds(cut, plane - cut)
    c_copy, x_copy, y2_copy, d_copy, a_copy = {}, {}, {}, {}, {}
    zk = {h: take(2 * slabs) for h in range(2)}
    chunk_rows = slabs * half_tok

    def down_act(h):
        for cc in range(2):
            for k in range(slabs):
                p = planes[k]
                for xx in range(2):
                    for yy in range(2):
                        source = c if cc == 0 else 1 - c
                        b = xx * 4 + yy * 2 + source
                        place = pl.ds(
                            pl.multiple_of((b * slabs + p) * half_tok, half_tok), half_tok
                        )
                        mean = jnp.sum(squares[h, place, :], axis=-1, keepdims=True)
                        scale = lax.rsqrt(mean * (1.0 / model) + 1e-06)
                        mine = gates[p, xx, yy, source, h * half_tok : (h + 1) * half_tok]
                        share = jnp.sum(
                            jnp.where(picked, mine.astype(F32), 0.0), axis=-1, keepdims=True
                        )
                        left = acc[h, place, :ff] * scale
                        right = acc[h, place, ff:] * (scale * share)
                        value = left / (1.0 + jnp.exp(-left)) * right
                        spot = ((cc * 2 + xx) * 2 + yy) * chunk_rows + k * half_tok
                        act[spot : spot + half_tok, :] = value.astype(BF16)
        if h == 0:
            loads[slabs].wait()

    def down_project(h, q):
        tile = plane // 2

        @pl.loop(2 * q, 2 * q + 2)
        def _(n):
            got = jnp.dot(
                act[...],
                down[:, pl.ds(pl.multiple_of(n * tile, tile), tile)],
                preferred_element_type=F32,
            ).astype(BF16)
            columns = pl.ds(pl.multiple_of((n % 2) * tile, tile), tile)
            for cc in range(2):
                for xx in range(2):
                    for yy in range(2):
                        spot = ((cc * 2 + xx) * 2 + yy) * chunk_rows
                        rows[q, xx, yy, 1 - cc, h, :, columns] = got[spot : spot + chunk_rows]

        c_copy[h, q] = send(rows.at[q, :, :, 0, h], got_core.at[q, :, :, h], core)

    def add_into(ref, other):
        count_rows = ref.shape[0]
        for start in range(0, count_rows, 32):
            spot = slice(start, start + 32)
            ref[spot, :] = (ref[spot, :].astype(F32) + other[spot, :].astype(F32)).astype(BF16)

    def add_cores(h, q):
        c_copy[h, q].wait_recv()
        for xx in range(2):
            for yy in range(2):
                add_into(rows.at[q, xx, yy, 1, h], got_core.at[q, xx, yy, h])
        x_copy[h, q] = send(rows.at[q, 1 - x, :, 1, h, :, part_d], got_x.at[q, :, h], over_x)
        y2_copy[h, q] = send(rows.at[q, :, 1 - y, 1, h, :, part_a], got_y2.at[q, :, h], over_y)

    def send_home(h, q, source, landing, index):
        for k in range(slabs - 1, 0, -1):
            Tracked(source(k), landing.at[z, h, q], zk[h] + index + z, device(planes[k], x, y, c))

    def landed(h, landing, index):
        for p in others:
            spot = landing.at[p, h]
            copy_of(spot, spot, 0, zk[h] + index + p, core).wait_recv()

    def add_a(h, q):
        y2_copy[h, q].wait_recv()
        for xx in range(2):
            add_into(rows.at[q, xx, y, 1, h, :, part_a], got_y2.at[q, xx, h])
        send_home(h, q, lambda k: rows.at[q, :, y, 1, h, spots(k), part_a], landed_a, 0)

    def add_d(h, q):
        x_copy[h, q].wait_recv()
        for yy in range(2):
            add_into(rows.at[q, x, yy, 1, h, :, part_d], got_x.at[q, yy, h])
        d_copy[h, q] = send(rows.at[q, x, 1 - y, 1, h, :, part_d], last_d.at[q, h], over_y)

    def add_last(h, q):
        d_copy[h, q].wait_recv()
        add_into(rows.at[q, x, y, 1, h, :, part_d], last_d.at[q, h])
        send_home(h, q, lambda k: rows.at[q, x, y, 1, h, spots(k), part_d], landed_d, slabs)

    def landed_sum(h):
        landed(h, landed_a, 0)
        for q in range(slabs):
            for xx in range(2):
                total = rows[q, xx, y, 1, h, spots(0), part_a].astype(F32)
                for p in others:
                    total = total + landed_a[p, h, q, xx].astype(F32)
                rows[q, xx, y, 1, h, spots(0), part_a] = total.astype(BF16)
        a_copy[h] = send(
            rows.at[:, 1 - x, y, 1, h, spots(0), part_a], last_a.at[h], over_x
        )

    def output(h):
        place = slice(h * half_tok, (h + 1) * half_tok)
        a_copy[h].wait_recv()
        for q in range(slabs):
            total = hidden[q, place, part_a].astype(F32)
            total = total + rows[q, x, y, 1, h, spots(0), part_a].astype(F32)
            total = total + last_a[h, q].astype(F32)
            out_ref[place, q * plane : q * plane + cut] = total.astype(BF16)
        landed(h, landed_d, slabs)
        for q in range(slabs):
            total = hidden[q, place, part_d].astype(F32)
            total = total + rows[q, x, y, 1, h, spots(0), part_d].astype(F32)
            for p in others:
                total = total + landed_d[p, h, q].astype(F32)
            out_ref[place, q * plane + cut : (q + 1) * plane] = total.astype(BF16)

    send_half(0)
    first(0, 0)
    first(1, 0)
    second_y(0, 0)
    second_x(0, 0)
    second_x(1, 0)
    second_y(1, 0)
    first(0, 1)
    send_half(1)
    third_y(0, 0)
    third_x(0, 0)
    gates_y()
    up_project(0, 0)
    first(0, 2)
    third_y(1, 0)
    third_x(1, 0)
    second_x(0, 1)
    second_y(0, 1)
    first(0, 3)
    gates_c()
    up_project(1, 0)
    second_y(0, 2)
    second_x(0, 2)
    first(1, 1)
    third_y(0, 1)
    third_x(0, 1)
    second_y(0, 3)
    second_x(0, 3)
    up_project(0, 1)
    first(1, 2)
    third_y(0, 2)
    third_x(0, 2)
    second_y(1, 1)
    second_x(1, 1)
    up_project(0, 2)
    first(1, 3)
    third_y(0, 3)
    third_x(0, 3)
    second_y(1, 2)
    second_x(1, 2)
    up_project(0, 3)
    gates_done()
    clear(0)
    down_act(0)
    third_x(1, 1)
    third_y(1, 1)
    down_project(0, 0)
    second_x(1, 3)
    second_y(1, 3)
    down_project(0, 1)
    down_project(0, 2)
    third_x(1, 2)
    third_y(1, 2)
    add_cores(0, 0)
    down_project(0, 3)
    add_cores(0, 1)
    up_project(1, 1)
    third_y(1, 3)
    third_x(1, 3)
    add_cores(0, 2)
    add_cores(0, 3)
    up_project(1, 2)
    add_a(0, 0)
    add_d(0, 0)
    add_a(0, 1)
    up_project(1, 3)
    add_a(0, 2)
    clear(1)
    down_act(1)
    add_d(0, 1)
    down_project(1, 0)
    add_a(0, 3)
    down_project(1, 1)
    add_last(0, 0)
    down_project(1, 2)
    add_d(0, 2)
    add_cores(1, 0)
    add_last(0, 1)
    down_project(1, 3)
    add_cores(1, 1)
    add_cores(1, 2)
    add_d(0, 3)
    add_cores(1, 3)
    add_last(0, 2)
    add_a(1, 0)
    add_d(1, 0)
    add_a(1, 1)
    add_a(1, 2)
    add_d(1, 1)
    add_last(0, 3)
    add_d(1, 2)
    add_a(1, 3)
    add_last(1, 0)
    add_last(1, 1)
    add_d(1, 3)
    landed_sum(0)
    add_last(1, 2)
    add_last(1, 3)
    landed_sum(1)
    output(0)
    output(1)
    for copy in pending:
        copy.wait_send()
    for i in range(chunks):
        chain_do(i, None, lambda copy: copy.wait_send())
        for p in others:
            chain_do(i, p, lambda copy: copy.wait_send())
    assert count[0] <= copies_max, count[0]


def layer(queries, keys, values, docs, out_proj, residual, gain, ids, weights, gate_up, down, groups):
    slabs = groups // 2
    tok, model = residual.shape
    tokens, depth = queries.shape
    plane = model // slabs
    ff, ff2 = down.shape[0], gate_up.shape[1]
    total = tok * slabs * 8
    half = slabs * tok // 2
    cut = 3 * plane // 8 // LANES * LANES
    copies_max = 88
    send_slots = 48
    dma = pltpu.SemaphoreType.DMA
    vmem = pl.BlockSpec(memory_space=pltpu.VMEM)
    hbm = pl.BlockSpec(memory_space=pl.ANY)
    return pl.pallas_call(
        functools.partial(layer_kernel, slabs, copies_max, send_slots),
        out_shape=jax.ShapeDtypeStruct((tok, model), BF16),
        in_specs=[hbm] * 3 + [vmem] + [hbm] * 2 + [vmem] * 3 + [hbm] * 2,
        out_specs=vmem,
        scratch_shapes=[
            pltpu.VMEM(queries.shape, BF16),
            pltpu.VMEM(keys.shape, BF16),
            pltpu.VMEM(values.shape, BF16),
            pltpu.VMEM(out_proj.shape, BF16),
            pltpu.VMEM(residual.shape, BF16),
            pltpu.VMEM((tokens, depth), BF16),
            pltpu.VMEM(out_proj.shape, BF16),
            pltpu.VMEM((slabs, tokens, depth), BF16),
            pltpu.VMEM((slabs, tok, plane), BF16),
            pltpu.VMEM((slabs, 2, 2, tok, plane), F32),
            pltpu.VMEM((slabs, 2, tok, plane), F32),
            pltpu.VMEM((slabs, tok, plane), BF16),
            pltpu.VMEM((slabs, tok, plane), BF16),
            pltpu.VMEM((ids.shape[0], LANES), jnp.int32),
            pltpu.VMEM((ids.shape[0], LANES), F32),
            pltpu.VMEM((slabs, 2, 2, 2, tok, LANES), BF16),
            pltpu.VMEM((slabs, 2, 2, 2, 2, half, plane), BF16),
            pltpu.VMEM((2, total // 2, LANES), F32),
            pltpu.VMEM((2, total // 2, ff2), F32),
            pltpu.VMEM((total // 2, ff), BF16),
            pltpu.VMEM((slabs, plane, ff2), BF16),
            pltpu.VMEM((ff, model), BF16),
            pltpu.VMEM((slabs, tok, plane), BF16),
            pltpu.VMEM((slabs, 2, 2, 2, half, plane), BF16),
            pltpu.VMEM((slabs, 2, 2, half, plane - cut), BF16),
            pltpu.VMEM((slabs, 2, 2, half, cut), BF16),
            pltpu.VMEM((slabs, 2, half, plane - cut), BF16),
            pltpu.VMEM((2, slabs, tok // 2, cut), BF16),
            pltpu.VMEM((slabs, 2, slabs, 2, tok // 2, cut), BF16),
            pltpu.VMEM((slabs, 2, slabs, tok // 2, plane - cut), BF16),
            dma((slabs + 6,)),
            dma((send_slots + 4 * (slabs + 2),)),
            dma((copies_max,)),
        ],
        compiler_params=pltpu.CompilerParams(
            collective_id=0, has_side_effects=True, vmem_limit_bytes=VMEM_LIMIT
        ),
    )(queries, keys, values, docs, out_proj, residual, gain, ids, weights, gate_up, down)


def spread_gates(expert_ids, gate_weights, experts):
    gates = jnp.sum(
        jnp.where(
            expert_ids[:, :, None] == jnp.arange(experts, dtype=jnp.int32)[None, None, :],
            gate_weights[:, :, None],
            0.0,
        ),
        axis=1,
    )
    high = lax.reduce_precision(gates, 8, 7)
    low = gates - high
    pad = -(2 * experts) % LANES
    return jnp.concatenate(
        [high, low, jnp.zeros((gates.shape[0], pad), F32)], axis=1
    ).astype(BF16)


def plain_layer(head_out, out_proj, residual, gain, extra, gate_up, down, groups, tensors):
    experts = groups * tensors
    tok, model = residual.shape
    heads = lax.all_gather(head_out, "group", axis=0, tiled=True)
    part = jnp.dot(heads, out_proj, preferred_element_type=F32)
    part = part.reshape(groups, tensors, tok, part.shape[1])
    part = lax.psum_scatter(part, "tensor", scatter_dimension=1, tiled=False)
    attended = lax.all_to_all(part, "group", split_axis=0, concat_axis=2, tiled=True)
    hidden = residual.astype(F32) + attended.reshape(tok, model)
    mean_square = jnp.mean(hidden * hidden, axis=-1, keepdims=True)
    normed = (hidden * lax.rsqrt(mean_square + 1e-06) * gain).astype(BF16)
    rows = jnp.concatenate([normed, extra], axis=1)
    rows_all = lax.all_gather(rows, ("group", "tensor"), axis=0, tiled=True)
    me = lax.axis_index("group") * tensors + lax.axis_index("tensor")
    lane = jnp.arange(extra.shape[1], dtype=jnp.int32)
    picked = (lane == me) | (lane == me + experts)
    gate_col = jnp.sum(
        jnp.where(picked[None, :], rows_all[:, model:].astype(F32), 0.0), axis=1, keepdims=True
    )
    ff = down.shape[0]
    projected = jnp.dot(rows_all[:, :model], gate_up, preferred_element_type=F32)
    activated = (jax.nn.silu(projected[:, :ff]) * projected[:, ff:]).astype(BF16)
    expert_out = jnp.dot(activated, down, preferred_element_type=F32)
    weighted = (expert_out * gate_col).astype(BF16)
    expert_sum = lax.psum_scatter(weighted, ("group", "tensor"), scatter_dimension=0, tiled=True)
    return (hidden + expert_sum.astype(F32)).astype(BF16)


def on_device(
    queries,
    keys,
    values,
    document_index,
    out_proj,
    residual_in,
    norm_gain,
    expert_ids,
    gate_weights,
    w_gate_up,
    w_down,
):
    groups, tensors = lax.axis_size("group"), lax.axis_size("tensor")
    gain = norm_gain[None, :]
    if groups == 8 and tensors == 4:
        return layer(
            queries,
            keys,
            values,
            document_index,
            out_proj,
            residual_in,
            gain,
            expert_ids.T,
            gate_weights.T,
            w_gate_up[0],
            w_down[0],
            groups,
        )
    head_out = attention(queries, keys, values, document_index)
    extra = spread_gates(expert_ids, gate_weights, groups * tensors)
    return plain_layer(
        head_out, out_proj, residual_in, gain, extra, w_gate_up[0], w_down[0], groups, tensors
    )


def solution(mesh):
    in_specs = (
        P("group", "tensor"),
        P("group", "tensor"),
        P("group", "tensor"),
        P("group", None),
        P("tensor", "group"),
        P(("group", "tensor"), None),
        P(),
        P(("group", "tensor"), None),
        P(("group", "tensor"), None),
        P(("group", "tensor"), None, None),
        P(("group", "tensor"), None, None),
    )
    out_specs = P(("group", "tensor"), None)
    return jax.shard_map(
        on_device, mesh=mesh, in_specs=in_specs, out_specs=out_specs, check_vma=False
    )
```
